32 devices in a mesh: rep: 2 (over y), blk: 8 (over z, x), head: 2 (over core).
Axes of the slice: x: 2, y: 2, z: 4, core: 2. Of those that a mesh axis runs over, the one named last changes fastest.
Arguments:
- queries: bfloat16 [2, 512, 8192], P('rep', 'blk', 'head'), parts along dimension 0, may hold values from -200 to 200
- keys: bfloat16 [2, 512, 512], P('rep', 'blk', 'head'), parts along dimension 0, may hold values from -6 to 6
- values: bfloat16 [2, 512, 512], P('rep', 'blk', 'head'), parts along dimension 0, may hold values from -6 to 6
- prompt_length: int32 [2], P('rep'), parts along dimension 0, may hold values from 256 to 512
- span_order: int32 [32], P('rep'), parts along dimension 0, may hold values from 0 to 15, as said below
Outputs:
- attended: bfloat16 [2, 512, 8192], P('rep', 'blk', 'head'), parts along dimension 0
The draws below stay inside these ranges and needn't reach their ends.
There are 2 independent parts, one for each index of `rep`. The reference program is written for one: setup_inputs(seed, part) draws one part's arguments, and reference() takes and returns one part's arrays. A program takes and returns all parts, laid end to end along the dimension named above; each array names one. Nothing has to cross between parts.
Inputs may be any that keep to these rules, and one draw needn't show every extreme that they name: `span_order`: each of the 16 span numbers stands in exactly one slot.
All inputs are finite; a program needn't handle non-finite values.
Results may differ from the reference program's by a relative error of at most 0.0065.
Values may be sent and summed in bfloat16 or wider, within the bound.
A program may use at most 64 MiB of HBM per device.

```python
import jax
import jax.numpy as jnp
from jax import lax

CH = 32
REPLICA_PROMPTS = 1
KEY_VALUE_HEADS = 4
QUERY_PER_KV = 16
HEAD_WIDTH = 128
NCHUNK = 16
PROMPT_TOKENS = 512


def span_table(key):
    return jax.random.permutation(jax.random.fold_in(key, 11), NCHUNK).astype(jnp.int32)


def draw_span_order(key, part):
    return span_table(key)


def base_keys(key):
    unscaled_scores = jax.random.normal(jax.random.fold_in(key, 23), (REPLICA_PROMPTS, PROMPT_TOKENS, KEY_VALUE_HEADS, HEAD_WIDTH), jnp.float32)
    return jnp.clip(unscaled_scores, -6.0, 6.0)


def draw_keys(key, part):
    unscaled_scores = base_keys(key)
    return unscaled_scores.reshape(REPLICA_PROMPTS, PROMPT_TOKENS, KEY_VALUE_HEADS * HEAD_WIDTH).astype(jnp.bfloat16)


def draw_queries(key, part):
    unscaled_scores = jax.random.normal(jax.random.fold_in(key, 31), (REPLICA_PROMPTS, PROMPT_TOKENS, KEY_VALUE_HEADS, QUERY_PER_KV, HEAD_WIDTH), jnp.float32)
    unscaled_scores = jnp.clip(unscaled_scores, -6.0, 6.0)
    return unscaled_scores.reshape(REPLICA_PROMPTS, PROMPT_TOKENS, KEY_VALUE_HEADS * QUERY_PER_KV * HEAD_WIDTH).astype(jnp.bfloat16)


def block_levels(key, dims, cuts, low, high):
    gain, own = 1.0, jax.random.fold_in(key, 6)
    for dim, shards_of in cuts:
        draws = jnp.exp(jax.random.uniform(jax.random.fold_in(own, dim), (shards_of,), jnp.float32, low / len(cuts), high / len(cuts)))
        gain = gain * jnp.repeat(draws, dims[dim] // shards_of).reshape([-1 if axis == dim else 1 for axis in range(len(dims))])
    return gain


def normal_values(key, shape, width, bound, pieces=(), held_as=jnp.bfloat16):
    entries = jax.random.normal(key, shape, jnp.float32) * width
    if len(pieces) > 0:
        entries = block_levels(key, shape, pieces, -0.22, 0.18) * entries
    return jnp.clip(entries, min=-bound, max=bound).astype(held_as)


def setup_inputs(seed: int = 0, part: int = 0) -> dict:
    key_list = jax.random.split(jax.random.key(seed), 6)
    part_splits = jax.random.split(jax.random.fold_in(key_list[5], part), 6)
    queries = draw_queries(jax.random.fold_in(jax.random.fold_in(key_list[5], part), 71), part)
    keys = draw_keys(jax.random.fold_in(jax.random.fold_in(key_list[5], part), 71), part)
    values = normal_values(part_splits[2], (REPLICA_PROMPTS, PROMPT_TOKENS, KEY_VALUE_HEADS * HEAD_WIDTH), 1.0, 6.0, ((1, 8), (2, 2)))
    prompt_length = jax.random.randint(part_splits[3], (REPLICA_PROMPTS,), PROMPT_TOKENS // 2, PROMPT_TOKENS + 1).astype(jnp.int32)
    span_order = draw_span_order(jax.random.fold_in(jax.random.fold_in(key_list[5], part), 71), part)
    return {"queries": queries, "keys": keys, "values": values, "prompt_length": prompt_length, "span_order": span_order}


NEG_FILL = -1e30


def one_prompt(queries, keys, values, limit, position):
    allowed = (position[None, :] <= position[:, None]) & (position[None, :] < limit)
    query_heads = queries.reshape(PROMPT_TOKENS, KEY_VALUE_HEADS, QUERY_PER_KV, HEAD_WIDTH).transpose(1, 2, 0, 3).reshape(KEY_VALUE_HEADS * QUERY_PER_KV, PROMPT_TOKENS, HEAD_WIDTH)
    key_heads = jnp.repeat(keys.reshape(PROMPT_TOKENS, KEY_VALUE_HEADS, HEAD_WIDTH).transpose(1, 0, 2), QUERY_PER_KV, axis=0)
    value_heads = jnp.repeat(values.reshape(PROMPT_TOKENS, KEY_VALUE_HEADS, HEAD_WIDTH).transpose(1, 0, 2), QUERY_PER_KV, axis=0)
    scale = HEAD_WIDTH ** -0.5

    def one_head(parts):
        query, key_rows, value_rows = parts
        scores = jnp.dot(query, key_rows.T, preferred_element_type=jnp.float32) * scale
        scores = jnp.where(allowed, scores, NEG_FILL)
        top = jnp.max(scores, axis=1, keepdims=True)
        weights = jnp.where(allowed, jnp.exp(scores - top), 0.0)
        total = jnp.sum(weights, axis=1, keepdims=True)
        mixed = jnp.dot(weights.astype(jnp.bfloat16), value_rows, preferred_element_type=jnp.float32)
        return mixed / total

    head_results = lax.map(one_head, (query_heads, key_heads, value_heads))
    joined_heads = head_results.reshape(KEY_VALUE_HEADS, QUERY_PER_KV, PROMPT_TOKENS, HEAD_WIDTH).transpose(2, 0, 1, 3).reshape(PROMPT_TOKENS, KEY_VALUE_HEADS * QUERY_PER_KV * HEAD_WIDTH)
    joined_heads = jnp.where((position < limit)[:, None], joined_heads, 0.0)
    return joined_heads.astype(jnp.bfloat16)


def reference(queries, keys, values, prompt_length, span_order):
    offsets = jnp.arange(CH, dtype=jnp.int32)
    position = (span_order[:, None].astype(jnp.int32) * CH + offsets[None, :]).reshape(-1).astype(jnp.int32)
    outputs = []
    for index in range(REPLICA_PROMPTS):
        outputs.append(one_prompt(queries[index], keys[index], values[index], prompt_length[index], position))
    return jnp.stack(outputs)
```

```python
import functools
import math

import jax
import jax.numpy as jnp
from jax import lax
from jax.experimental import pallas as pl
from jax.experimental.pallas import tpu as pltpu
from jax.sharding import PartitionSpec as P

HEAD_WIDTH = 128
NEG_FILL = -1e30
HEADS_PER_TILE = 2
KEY_CHUNK = 512
OUT_PARTS = 2
VMEM_LIMIT = 40 * 1024 * 1024
MESH = pl.DeviceIdType.MESH


def row_length(blocks):
    return max(d for d in range(1, math.isqrt(blocks) + 1) if blocks % d == 0)


def positions(order_ref, first, spans, span, shape, axis):
    index = lax.broadcasted_iota(jnp.int32, shape, axis)
    position = jnp.zeros(shape, jnp.int32)
    for t in range(spans):
        position = jnp.where(index // span == t, order_ref[first + t] * span + index % span, position)
    return position


def fill_bias(bias_ref, order_ref, limit, row_pos, span):
    chunks, _, chunk = bias_ref.shape
    spans = chunk // span

    def make(c):
        key_pos = positions(order_ref, c * spans, spans, span, (1, chunk), 1)
        bias_ref[c] = jnp.where((key_pos <= row_pos) & (key_pos < limit), 0.0, NEG_FILL)

    pl.loop(0, chunks)(make)


def exchange(rows_z, cols_x, refs, loads, ready_z, ready_x, z_send, x_send, recv):
    blocks = rows_z * cols_x
    rows = refs[0].shape[0] // blocks
    me = lax.axis_index("blk")
    z, x = lax.div(me, cols_x), lax.rem(me, cols_x)

    def copy(u, row, col, to_row, to_col, send):
        at = pl.ds((row * cols_x + col) * rows, rows)
        return pltpu.make_async_remote_copy(
            src_ref=refs[u].at[at],
            dst_ref=refs[u].at[at],
            send_sem=send,
            recv_sem=recv.at[row, col, u],
            device_id={"blk": to_row * cols_x + to_col},
            device_id_type=MESH,
        )

    def z_copy(row, u):
        return copy(u, z, x, row, x, z_send.at[row, u])

    def x_copy(row, col, u):
        return copy(u, row, x, z, col, x_send.at[row, col, u])

    def above(d, visit):
        pl.when(z + d < rows_z)(lambda: visit(z + d))

    def below(d, visit):
        pl.when(z >= d)(lambda: visit(z - d))

    def right(visit):
        for e in range(1, cols_x):
            pl.when(x + e < cols_x)(lambda e=e: visit(x + e))

    def left(visit):
        for e in range(1, cols_x):
            pl.when(x >= e)(lambda e=e: visit(x - e))

    far = range(rows_z - 1, 0, -1)
    near = range(1, rows_z)
    barrier = pltpu.get_barrier_semaphore()

    def signal(sem, row, col):
        pl.semaphore_signal(sem, inc=1, device_id={"blk": row * cols_x + col}, device_id_type=MESH)

    for d in near:
        above(d, lambda row: signal(barrier, row, x))
    right(lambda col: signal(barrier, z, col))
    pl.when(z + x > 0)(lambda: pl.semaphore_wait(barrier, z + x))
    for d in far:
        below(d, lambda row: signal(ready_z.at[z], row, x))
    left(lambda col: signal(ready_x.at[x], z, col))

    for u in range(2):
        loads[u].wait()
        for d in far:
            below(d, lambda row: z_copy(row, u).start())
        left(lambda col: x_copy(z, col, u).start())

    def send_right(col):
        pl.semaphore_wait(ready_x.at[col], 1)
        for u in range(2):
            x_copy(z, col, u).start()

    def send_above(row):
        pl.semaphore_wait(ready_z.at[row], 1)
        for u in range(2):
            z_copy(row, u).start()

    right(send_right)
    for d in near:
        above(d, send_above)

    def relay(row, u):
        copy(u, row, x, z, x, z_send.at[row, u]).wait_recv()
        right(lambda col: x_copy(row, col, u).start())
        left(lambda col: x_copy(row, col, u).start())

    for u in range(2):
        for d in near:
            below(d, lambda row: relay(row, u))
            above(d, lambda row: relay(row, u))

    def arrived(u):
        for row in range(rows_z):
            def take(col, row=row):
                copy(u, row, col, z, x, x_send.at[row, x, u]).wait_recv()

            left(take)
            right(take)

    def drain():
        for u in range(2):
            for d in near:
                above(d, lambda row: z_copy(row, u).wait_send())
                below(d, lambda row: z_copy(row, u).wait_send())
            for row in range(rows_z):
                right(lambda col, row=row: x_copy(row, col, u).wait_send())
                left(lambda col, row=row: x_copy(row, col, u).wait_send())

    return arrived, drain


def own_loads(blocks, k_hbm, v_hbm, k_ref, v_ref, sem):
    rows = k_ref.shape[0] // blocks
    own = pl.ds(lax.axis_index("blk") * rows, rows)
    loads = [
        pltpu.make_async_copy(source.at[0], ref.at[own], sem.at[u])
        for u, (source, ref) in enumerate(((k_hbm, k_ref), (v_hbm, v_ref)))
    ]
    for load in loads:
        load.start()
    return loads


def gather_kernel(rows_z, cols_x, k_hbm, v_hbm, k_ref, v_ref, own_sem, *sems):
    loads = own_loads(rows_z * cols_x, k_hbm, v_hbm, k_ref, v_ref, own_sem)
    arrived, drain = exchange(rows_z, cols_x, (k_ref, v_ref), loads, *sems)
    arrived(0)
    arrived(1)
    drain()


def stacked_queries(q_ref, first, tile):
    def cols(t):
        return pl.ds(pl.multiple_of(first + t * HEAD_WIDTH, HEAD_WIDTH), HEAD_WIDTH)

    return cols, jnp.concatenate([q_ref[:, cols(t)] for t in range(tile)], axis=0)


def scores(q, keys, bias, tile):
    scale = HEAD_WIDTH ** (-0.5) * math.log2(math.e)
    score = lax.dot_general(q, keys, (((1,), (1,)), ((), ())), preferred_element_type=jnp.float32)
    rows, chunk = bias.shape
    return ((score * scale).reshape(tile, rows, chunk) + bias[None]).reshape(tile * rows, chunk)


def weight_kernel(
    rows_z, cols_x, group, spans, k_hbm, v_hbm, q_hbm, len_hbm, order_hbm, w_ref, v_ref, live_ref,
    q_ref, k_ref, bias_ref, len_ref, order_ref, q_sem, small_sem, own_sem, *sems
):
    loads = own_loads(rows_z * cols_x, k_hbm, v_hbm, k_ref, v_ref, own_sem)
    q_copy = pltpu.make_async_copy(q_hbm.at[0], q_ref, q_sem)
    len_copy = pltpu.make_async_copy(len_hbm, len_ref, small_sem.at[0])
    order_copy = pltpu.make_async_copy(order_hbm, order_ref, small_sem.at[1])
    len_copy.start()
    order_copy.start()
    q_copy.start()
    arrived, drain = exchange(rows_z, cols_x, (k_ref, v_ref), loads, *sems)

    rows = q_ref.shape[0]
    span = rows // spans
    len_copy.wait()
    order_copy.wait()
    limit = len_ref[0]
    row_pos = positions(order_ref, lax.axis_index("blk") * spans, spans, span, (rows, 1), 0)
    fill_bias(bias_ref, order_ref, limit, row_pos, span)
    live_ref[...] = jnp.broadcast_to(jnp.where(row_pos < limit, 1.0, 0.0), live_ref.shape)
    q_copy.wait()
    arrived(0)

    tile = HEADS_PER_TILE if group % HEADS_PER_TILE == 0 else 1
    height = tile * rows
    for h in range(k_ref.shape[1] // HEAD_WIDTH):
        cols = slice(h * HEAD_WIDTH, (h + 1) * HEAD_WIDTH)

        def weigh(i, h=h, cols=cols):
            _, q = stacked_queries(q_ref, (h * group + i * tile) * HEAD_WIDTH, tile)
            score = scores(q, k_ref[:, cols], bias_ref[0], tile)
            top = jnp.max(score, axis=1, keepdims=True)
            kept = pl.ds(pl.multiple_of((h * (group // tile) + i) * height, height), height)
            w_ref[kept] = jnp.exp2(score - top).astype(jnp.bfloat16)

        pl.loop(0, group // tile, unroll=True)(weigh)
    arrived(1)
    drain()


def store_heads(o_ref, mixed, live, cols, tile):
    rows = live.shape[0]
    out = mixed[:, :HEAD_WIDTH] / mixed[:, HEAD_WIDTH:]
    for t in range(tile):
        o_ref[:, cols(t)] = jnp.where(live, out[t * rows : (t + 1) * rows], 0.0).astype(o_ref.dtype)


def with_ones(values):
    return jnp.concatenate([values, jnp.ones((values.shape[0], HEAD_WIDTH), values.dtype)], axis=1)


def in_parts(o_hbm, o_ref, out_sem, local_heads, group, tile, visit):
    tiles = group // tile
    per_part = tiles // OUT_PARTS
    wide = group * HEAD_WIDTH // OUT_PARTS
    copies = []
    for h in range(local_heads):
        for p in range(OUT_PARTS):
            pl.loop(p * per_part, (p + 1) * per_part, unroll=True)(lambda i, h=h: visit(h, i))
            at = pl.ds((h * OUT_PARTS + p) * wide, wide)
            copies.append(pltpu.make_async_copy(o_ref.at[:, at], o_hbm.at[0, :, at], out_sem.at[h, p]))
            copies[-1].start()
    for copy in copies:
        copy.wait()


def mix_kernel(group, w_ref, v_ref, live_ref, o_hbm, o_ref, out_sem):
    tile = HEADS_PER_TILE if group % HEADS_PER_TILE == 0 else 1
    height = tile * live_ref.shape[0]
    live = live_ref[...] > 0.0

    def visit(h, i):
        first = (h * group + i * tile) * HEAD_WIDTH
        kept = pl.ds(pl.multiple_of((h * (group // tile) + i) * height, height), height)
        values = with_ones(v_ref[:, h * HEAD_WIDTH : (h + 1) * HEAD_WIDTH])
        mixed = jnp.dot(w_ref[kept], values, preferred_element_type=jnp.float32)

        def cols(t):
            return pl.ds(pl.multiple_of(first + t * HEAD_WIDTH, HEAD_WIDTH), HEAD_WIDTH)

        store_heads(o_ref, mixed, live, cols, tile)

    in_parts(o_hbm, o_ref, out_sem, v_ref.shape[1] // HEAD_WIDTH, group, tile, visit)


def attend_kernel(
    group, spans, q_hbm, k_ref, v_ref, len_hbm, order_hbm, o_hbm,
    q_ref, o_ref, bias_ref, len_ref, order_ref, q_sem, small_sem, out_sem
):
    q_copy = pltpu.make_async_copy(q_hbm.at[0], q_ref, q_sem)
    len_copy = pltpu.make_async_copy(len_hbm, len_ref, small_sem.at[0])
    order_copy = pltpu.make_async_copy(order_hbm, order_ref, small_sem.at[1])
    for copy in (len_copy, order_copy, q_copy):
        copy.start()
    rows = q_ref.shape[0]
    span = rows // spans
    len_copy.wait()
    order_copy.wait()
    limit = len_ref[0]
    row_pos = positions(order_ref, lax.axis_index("blk") * spans, spans, span, (rows, 1), 0)
    fill_bias(bias_ref, order_ref, limit, row_pos, span)
    live = row_pos < limit
    q_copy.wait()
    tile = HEADS_PER_TILE if group % HEADS_PER_TILE == 0 else 1
    height = tile * rows
    chunks, _, chunk = bias_ref.shape

    def visit(h, i):
        cols = slice(h * HEAD_WIDTH, (h + 1) * HEAD_WIDTH)
        q_cols, q = stacked_queries(q_ref, (h * group + i * tile) * HEAD_WIDTH, tile)

        def step(c, state):
            best, mixed = state
            at = pl.ds(pl.multiple_of(c * chunk, chunk), chunk)
            score = scores(q, k_ref[at, cols], bias_ref[c], tile)
            top = jnp.maximum(best, jnp.max(score, axis=1, keepdims=True))
            weight = jnp.exp2(score - top).astype(jnp.bfloat16)
            fresh = jnp.dot(weight, with_ones(v_ref[at, cols]), preferred_element_type=jnp.float32)
            return top, mixed * jnp.exp2(best - top) + fresh

        init = (
            jnp.full((height, 1), NEG_FILL, jnp.float32),
            jnp.zeros((height, 2 * HEAD_WIDTH), jnp.float32),
        )
        _, mixed = lax.fori_loop(0, chunks, step, init)
        store_heads(o_ref, mixed, live, q_cols, tile)

    in_parts(o_hbm, o_ref, out_sem, k_ref.shape[1] // HEAD_WIDTH, group, tile, visit)


def solution(mesh):
    blocks = mesh.shape["blk"]
    cols_x = row_length(blocks)
    rows_z = blocks // cols_x
    dma = pltpu.SemaphoreType.DMA
    hbm = pl.BlockSpec(memory_space=pltpu.HBM)
    vmem = pl.BlockSpec(memory_space=pltpu.VMEM)

    def shards(queries, keys, values, prompt_length, span_order):
        _, rows, width = queries.shape
        kv_width = keys.shape[2]
        local_heads = kv_width // HEAD_WIDTH
        group = width // kv_width
        total = blocks * rows
        chunk = min(total, KEY_CHUNK)
        spans = span_order.shape[0] // blocks
        queries, keys, values, span_order = (
            pltpu.with_memory_space_constraint(a, pltpu.HBM) for a in (queries, keys, values, span_order)
        )
        exchange_sems = [
            dma((2,)),
            pltpu.SemaphoreType.REGULAR((rows_z,)),
            pltpu.SemaphoreType.REGULAR((cols_x,)),
            dma((rows_z, 2)),
            dma((rows_z, cols_x, 2)),
            dma((rows_z, cols_x, 2)),
        ]
        small = [pltpu.SMEM(prompt_length.shape, jnp.int32), pltpu.SMEM(span_order.shape, jnp.int32)]
        talk = pltpu.CompilerParams(collective_id=0, has_side_effects=True, vmem_limit_bytes=VMEM_LIMIT)
        quiet = pltpu.CompilerParams(vmem_limit_bytes=VMEM_LIMIT)
        out_shape = jax.ShapeDtypeStruct(queries.shape, queries.dtype)
        out_sems = dma((local_heads, OUT_PARTS))
        gathered = pltpu.VMEM((total, kv_width), keys.dtype)
        bias = pltpu.VMEM((total // chunk, rows, chunk), jnp.float32)
        wide = pltpu.VMEM((rows, width), queries.dtype)
        if chunk == total:
            parts = pl.pallas_call(
                functools.partial(weight_kernel, rows_z, cols_x, group, spans),
                out_shape=[
                    pltpu.VMEM((local_heads * group * rows, total), jnp.bfloat16),
                    gathered,
                    pltpu.VMEM((rows, HEAD_WIDTH), jnp.float32),
                ],
                in_specs=[hbm] * 5,
                out_specs=[vmem] * 3,
                scratch_shapes=[wide, gathered, bias, *small, dma, dma((2,)), *exchange_sems],
                compiler_params=talk,
            )(keys, values, queries, prompt_length, span_order)
            return pl.pallas_call(
                functools.partial(mix_kernel, group),
                out_shape=out_shape,
                in_specs=[vmem] * 3,
                out_specs=hbm,
                scratch_shapes=[wide, out_sems],
                compiler_params=quiet,
            )(*parts)
        k_all, v_all = pl.pallas_call(
            functools.partial(gather_kernel, rows_z, cols_x),
            out_shape=[gathered] * 2,
            in_specs=[hbm] * 2,
            out_specs=[vmem] * 2,
            scratch_shapes=exchange_sems,
            compiler_params=talk,
        )(keys, values)
        return pl.pallas_call(
            functools.partial(attend_kernel, group, spans),
            out_shape=out_shape,
            in_specs=[hbm, vmem, vmem, hbm, hbm],
            out_specs=hbm,
            scratch_shapes=[wide, wide, bias, *small, dma, dma((2,)), out_sems],
            compiler_params=quiet,
        )(queries, k_all, v_all, prompt_length, span_order)

    spec = P("rep", "blk", "head")
    return jax.shard_map(
        shards, mesh=mesh, in_specs=(spec, spec, spec, P("rep"), P("rep")), out_specs=spec, check_vma=False
    )
```

```python
import functools
import math

import jax
import jax.numpy as jnp
from jax import lax
from jax.experimental import pallas as pl
from jax.experimental.pallas import tpu as pltpu
from jax.sharding import PartitionSpec as P

HEAD_WIDTH = 128
NEG_FILL = -1e30
HEADS_PER_TILE = 2
KEY_CHUNK = 512
OUT_PARTS = 2
VMEM_LIMIT = 40 * 1024 * 1024
MESH = pl.DeviceIdType.MESH


def row_length(blocks):
    return max(d for d in range(1, math.isqrt(blocks) + 1) if blocks % d == 0)


def positions(order_ref, first, spans, span, shape, axis):
    index = lax.broadcasted_iota(jnp.int32, shape, axis)
    position = jnp.zeros(shape, jnp.int32)
    for t in range(spans):
        position = jnp.where(index // span == t, order_ref[first + t] * span + index % span, position)
    return position


def fill_bias(bias_ref, order_ref, row_pos, span):
    chunks, _, chunk = bias_ref.shape
    spans = chunk // span

    def make(c):
        key_pos = positions(order_ref, c * spans, spans, span, (1, chunk), 1)
        bias_ref[c] = jnp.where(key_pos <= row_pos, 0.0, NEG_FILL)

    pl.loop(0, chunks)(make)


def exchange(rows_z, cols_x, sources, refs, meanwhile, own_sem, ready_z, ready_x, z_send, x_send, z_recv, x_recv):
    rows = sources[0].shape[1]
    me = lax.axis_index("blk")
    z, x = lax.div(me, cols_x), lax.rem(me, cols_x)
    even = lax.rem(z, 2) == 0
    near = range(1, rows_z)
    far = range(rows_z - 1, 0, -1)
    own = pl.ds(me * rows, rows)
    loads = [pltpu.make_async_copy(sources[u].at[0], refs[u].at[own], own_sem.at[u]) for u in range(2)]
    for load in loads:
        load.start()
    meanwhile()

    def send(source, u, row, to_row, to_col, send_sem, recv_sem):
        at = pl.ds((row * cols_x + x) * rows, rows)
        return pltpu.make_async_remote_copy(
            src_ref=refs[u].at[at] if source is None else source,
            dst_ref=refs[u].at[at],
            send_sem=send_sem,
            recv_sem=recv_sem,
            device_id={"blk": to_row * cols_x + to_col},
            device_id_type=MESH,
        )

    def z_copy(row, to_row, u, source=None):
        return send(source, u, row, to_row, x, z_send.at[u], z_recv.at[row, u])

    def x_copy(row, col, u):
        return send(None, u, row, z, col, x_send.at[u], x_recv.at[u])

    def above(d, visit):
        pl.when(z + d < rows_z)(lambda: visit(z + d))

    def below(d, visit):
        pl.when(z >= d)(lambda: visit(z - d))

    def right(visit):
        for e in range(1, cols_x):
            pl.when(x + e < cols_x)(lambda e=e: visit(x + e))

    def left(visit):
        for e in range(1, cols_x):
            pl.when(x >= e)(lambda e=e: visit(x - e))

    def spread(row, u):
        for e in range(1, cols_x):
            x_copy(row, lax.rem(x + e, cols_x), u).start()

    def signal(sem, row, col):
        pl.semaphore_signal(sem, inc=1, device_id={"blk": row * cols_x + col}, device_id_type=MESH)

    barrier = pltpu.get_barrier_semaphore()
    for d in near:
        above(d, lambda row: signal(barrier, row, x))
    right(lambda col: signal(barrier, z, col))
    pl.when(z + x > 0)(lambda: pl.semaphore_wait(barrier, z + x))
    for d in far:
        below(d, lambda row: signal(ready_z.at[z], row, x))
    left(lambda col: signal(ready_x.at[x], z, col))

    def direct(d, visit):
        if d == 2:
            pl.when(even)(visit)
        else:
            visit()

    def send_below(u):
        for d in far:
            direct(d, lambda d=d: below(d, lambda row: z_copy(z, row, u, sources[u].at[0]).start()))

    def send_above(d, *which):
        def go(row):
            for u in which:
                z_copy(z, row, u, sources[u].at[0]).start()

        if d != 3:
            direct(d, lambda: above(d, go))

    def answered(d):
        above(d, lambda row: pl.semaphore_wait(ready_z.at[row], 1))

    def relay_from_below(d, u):
        def take(row):
            z_copy(row, z, u).wait_recv()
            if d == 1:
                pl.when(even & (z + 1 < rows_z))(lambda: z_copy(row, z + 1, u).start())
            if d == 2:
                above(1, lambda to_row: z_copy(row, to_row, u).start())
            spread(row, u)

        below(d, take)

    def relay_from_above(d, u):
        def take(row):
            z_copy(row, z, u).wait_recv()
            spread(row, u)
            if d == 1:
                pl.when(even & (z >= 1))(lambda: z_copy(row, z - 1, u).start())

        above(d, take)

    def relay(d, u):
        relay_from_below(d, u)
        relay_from_above(d, u)

    def send_left(u):
        loads[u].wait()
        left(lambda col: x_copy(z, col, u).start())

    def send_right(*which):
        right(lambda col: pl.semaphore_wait(ready_x.at[col], 1))
        for u in which:
            right(lambda col: x_copy(z, col, u).start())

    def eager():
        for u in range(2):
            send_below(u)
            send_left(u)
        send_right(0, 1)
        for d in near:
            answered(d)
            send_above(d, 0, 1)

        def lowest():
            for u in range(2):
                relay_from_above(1, u)
            for u in range(2):
                for d in near[1:]:
                    relay_from_above(d, u)

        def others():
            for u in range(2):
                for d in near:
                    relay(d, u)

        pl.when(z == 0)(lowest)
        pl.when(z > 0)(others)

    def patient():
        send_below(0)
        send_left(0)
        right(lambda col: pl.semaphore_wait(ready_x.at[col], 1))
        right(lambda col: x_copy(z, col, 0).start())
        send_left(1)
        right(lambda col: x_copy(z, col, 1).start())
        for d in near:
            answered(d)
            send_above(d, 0)
        for d in near:
            relay(d, 0)
            if d == 1:
                send_below(1)
                for further in near:
                    send_above(further, 1)
        for d in near:
            relay(d, 1)

    first = lax.axis_index("head") == 0
    pl.when(first)(eager)
    pl.when(~first)(patient)

    def many(u, count, sem):
        at = pl.ds(0, count * rows)
        return pltpu.make_async_copy(refs[u].at[at], refs[u].at[at], sem)

    along_x = (cols_x - 1) * rows_z

    def arrived(u):
        many(u, along_x, x_recv.at[u]).wait()

    def sent_along_z(row):
        count = rows_z - 1 - (row + 3 < rows_z)
        if row % 2 == 1:
            count -= (row >= 2) + (row + 2 < rows_z)
        elif 0 < row < rows_z - 1:
            count += 2
        return count + (row >= 2 and row + 1 < rows_z)

    def drain():
        for u in range(2):
            many(u, along_x, x_send.at[u]).wait()
            for row in range(rows_z):
                pl.when(z == row)(lambda row=row: many(u, sent_along_z(row), z_send.at[u]).wait())

    return arrived, drain


def gather_kernel(rows_z, cols_x, k_hbm, v_hbm, k_ref, v_ref, *sems):
    arrived, drain = exchange(rows_z, cols_x, (k_hbm, v_hbm), (k_ref, v_ref), lambda: None, *sems)
    arrived(0)
    arrived(1)
    drain()


def stacked_queries(q_ref, first, tile):
    def cols(t):
        return pl.ds(pl.multiple_of(first + t * HEAD_WIDTH, HEAD_WIDTH), HEAD_WIDTH)

    return cols, jnp.concatenate([q_ref[:, cols(t)] for t in range(tile)], axis=0)


def scores(q, keys, bias, tile):
    scale = HEAD_WIDTH ** (-0.5) * math.log2(math.e)
    score = lax.dot_general(q, keys, (((1,), (1,)), ((), ())), preferred_element_type=jnp.float32)
    rows, chunk = bias.shape
    return ((score * scale).reshape(tile, rows, chunk) + bias[None]).reshape(tile * rows, chunk)


def weight_kernel(
    rows_z, cols_x, group, spans, k_hbm, v_hbm, q_hbm, len_hbm, order_hbm, w_ref, v_ref, live_ref,
    q_ref, k_ref, bias_ref, len_ref, order_ref, q_sem, small_sem, *sems
):
    q_copy = pltpu.make_async_copy(q_hbm.at[0], q_ref, q_sem)
    len_copy = pltpu.make_async_copy(len_hbm, len_ref, small_sem.at[0])
    order_copy = pltpu.make_async_copy(order_hbm, order_ref, small_sem.at[1])
    copies = (len_copy, order_copy, q_copy)
    arrived, drain = exchange(
        rows_z, cols_x, (k_hbm, v_hbm), (k_ref, v_ref), lambda: [copy.start() for copy in copies], *sems
    )

    rows = q_ref.shape[0]
    span = rows // spans
    len_copy.wait()
    order_copy.wait()
    limit = len_ref[0]
    row_pos = positions(order_ref, lax.axis_index("blk") * spans, spans, span, (rows, 1), 0)
    fill_bias(bias_ref, order_ref, row_pos, span)
    live_ref[...] = jnp.broadcast_to(jnp.where(row_pos < limit, 1.0, 0.0), live_ref.shape)
    q_copy.wait()
    arrived(0)

    tile = HEADS_PER_TILE if group % HEADS_PER_TILE == 0 else 1
    height = tile * rows
    for h in range(k_ref.shape[1] // HEAD_WIDTH):
        cols = slice(h * HEAD_WIDTH, (h + 1) * HEAD_WIDTH)

        def weigh(i, h=h, cols=cols):
            _, q = stacked_queries(q_ref, (h * group + i * tile) * HEAD_WIDTH, tile)
            score = scores(q, k_ref[:, cols], bias_ref[0], tile)
            top = jnp.max(score, axis=1, keepdims=True)
            kept = pl.ds(pl.multiple_of((h * (group // tile) + i) * height, height), height)
            w_ref[kept] = jnp.exp2(score - top).astype(jnp.bfloat16)

        pl.loop(0, group // tile, unroll=True)(weigh)
    arrived(1)
    drain()


def store_heads(o_ref, mixed, live, cols, tile):
    rows = live.shape[0]
    out = mixed[:, :HEAD_WIDTH] / mixed[:, HEAD_WIDTH:]
    for t in range(tile):
        o_ref[:, cols(t)] = jnp.where(live, out[t * rows : (t + 1) * rows], 0.0).astype(o_ref.dtype)


def with_ones(values):
    return jnp.concatenate([values, jnp.ones((values.shape[0], HEAD_WIDTH), values.dtype)], axis=1)


def in_parts(o_hbm, o_ref, out_sem, local_heads, group, tile, visit, unroll):
    tiles = group // tile
    per_part = tiles // OUT_PARTS
    wide = group * HEAD_WIDTH // OUT_PARTS
    copies = []
    for h in range(local_heads):
        for p in range(OUT_PARTS):
            pl.loop(p * per_part, (p + 1) * per_part, unroll=unroll)(lambda i, h=h: visit(h, i))
            at = pl.ds((h * OUT_PARTS + p) * wide, wide)
            copies.append(pltpu.make_async_copy(o_ref.at[:, at], o_hbm.at[0, :, at], out_sem.at[h, p]))
            copies[-1].start()
    for copy in copies:
        copy.wait()


def mix_kernel(group, w_ref, v_ref, live_ref, o_hbm, o_ref, out_sem):
    tile = HEADS_PER_TILE if group % HEADS_PER_TILE == 0 else 1
    height = tile * live_ref.shape[0]
    live = live_ref[...] > 0.0

    def visit(h, i):
        first = (h * group + i * tile) * HEAD_WIDTH
        kept = pl.ds(pl.multiple_of((h * (group // tile) + i) * height, height), height)
        values = with_ones(v_ref[:, h * HEAD_WIDTH : (h + 1) * HEAD_WIDTH])
        mixed = jnp.dot(w_ref[kept], values, preferred_element_type=jnp.float32)

        def cols(t):
            return pl.ds(pl.multiple_of(first + t * HEAD_WIDTH, HEAD_WIDTH), HEAD_WIDTH)

        store_heads(o_ref, mixed, live, cols, tile)

    in_parts(o_hbm, o_ref, out_sem, v_ref.shape[1] // HEAD_WIDTH, group, tile, visit, True)


def attend_kernel(
    group, spans, q_hbm, k_ref, v_ref, len_hbm, order_hbm, o_hbm,
    q_ref, o_ref, bias_ref, len_ref, order_ref, q_sem, small_sem, out_sem
):
    q_copy = pltpu.make_async_copy(q_hbm.at[0], q_ref, q_sem)
    len_copy = pltpu.make_async_copy(len_hbm, len_ref, small_sem.at[0])
    order_copy = pltpu.make_async_copy(order_hbm, order_ref, small_sem.at[1])
    for copy in (len_copy, order_copy, q_copy):
        copy.start()
    rows = q_ref.shape[0]
    span = rows // spans
    len_copy.wait()
    order_copy.wait()
    limit = len_ref[0]
    row_pos = positions(order_ref, lax.axis_index("blk") * spans, spans, span, (rows, 1), 0)
    fill_bias(bias_ref, order_ref, row_pos, span)
    live = row_pos < limit
    q_copy.wait()
    tile = HEADS_PER_TILE if group % HEADS_PER_TILE == 0 else 1
    height = tile * rows
    chunks, _, chunk = bias_ref.shape

    def visit(h, i):
        cols = slice(h * HEAD_WIDTH, (h + 1) * HEAD_WIDTH)
        q_cols, q = stacked_queries(q_ref, (h * group + i * tile) * HEAD_WIDTH, tile)

        def step(c, state):
            best, mixed = state
            at = pl.ds(pl.multiple_of(c * chunk, chunk), chunk)
            score = scores(q, k_ref[at, cols], bias_ref[c], tile)
            top = jnp.maximum(best, jnp.max(score, axis=1, keepdims=True))
            weight = jnp.exp2(score - top).astype(jnp.bfloat16)
            fresh = jnp.dot(weight, with_ones(v_ref[at, cols]), preferred_element_type=jnp.float32)
            return top, mixed * jnp.exp2(best - top) + fresh

        init = (
            jnp.full((height, 1), NEG_FILL, jnp.float32),
            jnp.zeros((height, 2 * HEAD_WIDTH), jnp.float32),
        )
        _, mixed = lax.fori_loop(0, chunks, step, init)
        store_heads(o_ref, mixed, live, q_cols, tile)

    in_parts(o_hbm, o_ref, out_sem, k_ref.shape[1] // HEAD_WIDTH, group, tile, visit, False)


def solution(mesh):
    blocks = mesh.shape["blk"]
    cols_x = row_length(blocks)
    rows_z = blocks // cols_x
    dma = pltpu.SemaphoreType.DMA
    hbm = pl.BlockSpec(memory_space=pltpu.HBM)
    vmem = pl.BlockSpec(memory_space=pltpu.VMEM)

    def shards(queries, keys, values, prompt_length, span_order):
        _, rows, width = queries.shape
        kv_width = keys.shape[2]
        local_heads = kv_width // HEAD_WIDTH
        group = width // kv_width
        total = blocks * rows
        chunk = min(total, KEY_CHUNK)
        spans = span_order.shape[0] // blocks
        queries, keys, values, span_order = (
            pltpu.with_memory_space_constraint(a, pltpu.HBM) for a in (queries, keys, values, span_order)
        )
        exchange_sems = [
            dma((2,)),
            pltpu.SemaphoreType.REGULAR((rows_z,)),
            pltpu.SemaphoreType.REGULAR((cols_x,)),
            dma((2,)),
            dma((2,)),
            dma((rows_z, 2)),
            dma((2,)),
        ]
        small = [pltpu.SMEM(prompt_length.shape, jnp.int32), pltpu.SMEM(span_order.shape, jnp.int32)]
        talk = pltpu.CompilerParams(collective_id=0, has_side_effects=True, vmem_limit_bytes=VMEM_LIMIT)
        quiet = pltpu.CompilerParams(vmem_limit_bytes=VMEM_LIMIT)
        out_shape = jax.ShapeDtypeStruct(queries.shape, queries.dtype)
        out_sems = dma((local_heads, OUT_PARTS))
        gathered = pltpu.VMEM((total, kv_width), keys.dtype)
        bias = pltpu.VMEM((total // chunk, rows, chunk), jnp.float32)
        wide = pltpu.VMEM((rows, width), queries.dtype)
        if chunk == total:
            parts = pl.pallas_call(
                functools.partial(weight_kernel, rows_z, cols_x, group, spans),
                out_shape=[
                    pltpu.VMEM((local_heads * group * rows, total), jnp.bfloat16),
                    gathered,
                    pltpu.VMEM((rows, HEAD_WIDTH), jnp.float32),
                ],
                in_specs=[hbm] * 5,
                out_specs=[vmem] * 3,
                scratch_shapes=[wide, gathered, bias, *small, dma, dma((2,)), *exchange_sems],
                compiler_params=talk,
            )(keys, values, queries, prompt_length, span_order)
            return pl.pallas_call(
                functools.partial(mix_kernel, group),
                out_shape=out_shape,
                in_specs=[vmem] * 3,
                out_specs=hbm,
                scratch_shapes=[wide, out_sems],
                compiler_params=quiet,
            )(*parts)
        k_all, v_all = pl.pallas_call(
            functools.partial(gather_kernel, rows_z, cols_x),
            out_shape=[gathered] * 2,
            in_specs=[hbm] * 2,
            out_specs=[vmem] * 2,
            scratch_shapes=exchange_sems,
            compiler_params=talk,
        )(keys, values)
        return pl.pallas_call(
            functools.partial(attend_kernel, group, spans),
            out_shape=out_shape,
            in_specs=[hbm, vmem, vmem, hbm, hbm],
            out_specs=hbm,
            scratch_shapes=[wide, wide, bias, *small, dma, dma((2,)), out_sems],
            compiler_params=quiet,
        )(queries, k_all, v_all, prompt_length, span_order)

    spec = P("rep", "blk", "head")
    return jax.shard_map(
        shards, mesh=mesh, in_specs=(spec, spec, spec, P("rep"), P("rep")), out_specs=spec, check_vma=False
    )
```

```python
import functools
import math

import jax
import jax.numpy as jnp
from jax import lax
from jax.experimental import pallas as pl
from jax.experimental.pallas import tpu as pltpu
from jax.sharding import PartitionSpec as P

HEAD_WIDTH = 128
NEG_FILL = -1e30
HEADS_PER_TILE = 2
KEY_CHUNK = 512
OUT_PARTS = 2
VMEM_LIMIT = 40 * 1024 * 1024
MESH = pl.DeviceIdType.MESH


def row_length(blocks):
    return max(d for d in range(1, math.isqrt(blocks) + 1) if blocks % d == 0)


def row_positions(order_ref, spans, rows):
    span = rows // spans
    index = lax.broadcasted_iota(jnp.int32, (rows, 1), 0)
    position = jnp.zeros((rows, 1), jnp.int32)
    for t in range(spans):
        first = order_ref[lax.axis_index("blk") * spans + t] * span
        position = jnp.where(index // span == t, first + index % span, position)
    return position


def key_positions(order_ref, first_block, shape, rows_z, cols_x, spans, rows):
    span = rows // spans
    index = lax.broadcasted_iota(jnp.int32, shape, 1)
    position = jnp.zeros(shape, jnp.int32)
    for t in range(shape[1] // span):
        slot = first_block + t // spans
        block = lax.rem(slot, rows_z) * cols_x + lax.div(slot, rows_z)
        first = order_ref[block * spans + t % spans] * span
        position = jnp.where(index // span == t, first + index % span, position)
    return position


def mask(key_pos, row_pos):
    return jnp.where(key_pos <= row_pos, 0.0, NEG_FILL)


def exchange(rows_z, cols_x, sources, refs, meanwhile, prepare, own_keys, own_sem, ready_z, ready_x, z_send, x_send, z_recv, x_recv):
    rows = sources[0].shape[1]
    me = lax.axis_index("blk")
    z, x = lax.div(me, cols_x), lax.rem(me, cols_x)
    even = lax.rem(z, 2) == 0
    near = range(1, rows_z)
    far = range(rows_z - 1, 0, -1)
    own = pl.ds((x * rows_z + z) * rows, rows)
    loads = [pltpu.make_async_copy(sources[u].at[0], refs[u].at[own], own_sem.at[u]) for u in range(2)]
    for load in loads:
        load.start()
    meanwhile()

    def send(source, u, row, to_row, to_col, send_sem, recv_sem):
        at = pl.ds((x * rows_z + row) * rows, rows)
        return pltpu.make_async_remote_copy(
            src_ref=refs[u].at[at] if source is None else source,
            dst_ref=refs[u].at[at],
            send_sem=send_sem,
            recv_sem=recv_sem,
            device_id={"blk": to_row * cols_x + to_col},
            device_id_type=MESH,
        )

    def z_copy(row, to_row, u, source=None):
        return send(source, u, row, to_row, x, z_send.at[u], z_recv.at[row, u])

    def x_copy(row, col, u):
        return send(None, u, row, z, col, x_send.at[u], x_recv.at[u])

    def above(d, visit):
        pl.when(z + d < rows_z)(lambda: visit(z + d))

    def below(d, visit):
        pl.when(z >= d)(lambda: visit(z - d))

    def right(visit):
        for e in range(1, cols_x):
            pl.when(x + e < cols_x)(lambda e=e: visit(x + e))

    def left(visit):
        for e in range(1, cols_x):
            pl.when(x >= e)(lambda e=e: visit(x - e))

    def spread(row, u):
        for e in range(1, cols_x):
            x_copy(row, lax.rem(x + e, cols_x), u).start()

    def signal(sem, row, col):
        pl.semaphore_signal(sem, inc=1, device_id={"blk": row * cols_x + col}, device_id_type=MESH)

    barrier = pltpu.get_barrier_semaphore()
    for d in near:
        above(d, lambda row: signal(barrier, row, x))
    right(lambda col: signal(barrier, z, col))
    pl.when(z + x > 0)(lambda: pl.semaphore_wait(barrier, z + x))
    for d in far:
        below(d, lambda row: signal(ready_z.at[z], row, x))
    left(lambda col: signal(ready_x.at[x], z, col))

    def direct(d, visit):
        if d == 2:
            pl.when(even)(visit)
        else:
            visit()

    def send_below(u):
        for d in far:
            direct(d, lambda d=d: below(d, lambda row: z_copy(z, row, u, sources[u].at[0]).start()))

    def send_above(d, *which):
        def go(row):
            for u in which:
                z_copy(z, row, u, sources[u].at[0]).start()

        if d != 3:
            direct(d, lambda: above(d, go))

    def answered(d):
        above(d, lambda row: pl.semaphore_wait(ready_z.at[row], 1))

    def relay_from_below(d, u):
        def take(row):
            z_copy(row, z, u).wait_recv()
            if d == 1:
                pl.when(even & (z + 1 < rows_z))(lambda: z_copy(row, z + 1, u).start())
            if d == 2:
                above(1, lambda to_row: z_copy(row, to_row, u).start())
            spread(row, u)

        below(d, take)

    def relay_from_above(d, u):
        def take(row):
            z_copy(row, z, u).wait_recv()
            spread(row, u)
            if d == 1:
                pl.when(even & (z >= 1))(lambda: z_copy(row, z - 1, u).start())

        above(d, take)

    def relay(d, u):
        relay_from_below(d, u)
        relay_from_above(d, u)

    def send_left(u):
        loads[u].wait()
        left(lambda col: x_copy(z, col, u).start())

    def send_right(*which):
        right(lambda col: pl.semaphore_wait(ready_x.at[col], 1))
        for u in which:
            right(lambda col: x_copy(z, col, u).start())

    def eager():
        for u in range(2):
            send_below(u)
            send_left(u)
        send_right(0, 1)
        for d in near:
            answered(d)
            send_above(d, 0, 1)

    def patient():
        send_below(0)
        send_left(0)
        send_left(1)
        send_right(0, 1)
        for d in near:
            answered(d)
            send_above(d, 0)

    first = lax.axis_index("head") == 0
    pl.when(first)(eager)
    pl.when(~first)(patient)
    prepare()
    lowest = first & (z == 0)

    def values_now():
        send_below(1)
        for d in near:
            send_above(d, 1)

    for d in near:
        relay(d, 0)
        if d == 1:
            pl.when(lowest)(lambda: relay_from_above(1, 1))
            pl.when(~first)(values_now)
    for d in near:
        relay_from_below(d, 1)
        if d == 1:
            pl.when(~lowest)(lambda: relay_from_above(1, 1))
        else:
            relay_from_above(d, 1)
    own_keys()

    def many(u, count, sem):
        at = pl.ds(0, count * rows)
        return pltpu.make_async_copy(refs[u].at[at], refs[u].at[at], sem)

    along_x = (cols_x - 1) * rows_z

    def arrived(u):
        many(u, along_x, x_recv.at[u]).wait()

    def sent_along_z(row):
        count = rows_z - 1 - (row + 3 < rows_z)
        if row % 2 == 1:
            count -= (row >= 2) + (row + 2 < rows_z)
        elif 0 < row < rows_z - 1:
            count += 2
        return count + (row >= 2 and row + 1 < rows_z)

    def drain():
        for u in range(2):
            many(u, along_x, x_send.at[u]).wait()
            for row in range(rows_z):
                pl.when(z == row)(lambda row=row: many(u, sent_along_z(row), z_send.at[u]).wait())

    return arrived, drain


def gather_kernel(rows_z, cols_x, k_hbm, v_hbm, k_ref, v_ref, *sems):
    arrived, drain = exchange(rows_z, cols_x, (k_hbm, v_hbm), (k_ref, v_ref), *[lambda: None] * 3, *sems)
    arrived(0)
    arrived(1)
    drain()


def stacked_queries(q_ref, first, tile):
    def cols(t):
        return pl.ds(pl.multiple_of(first + t * HEAD_WIDTH, HEAD_WIDTH), HEAD_WIDTH)

    return cols, jnp.concatenate([q_ref[:, cols(t)] for t in range(tile)], axis=0)


def scores(q, keys, bias, tile):
    scale = HEAD_WIDTH ** (-0.5) * math.log2(math.e)
    score = lax.dot_general(q, keys, (((1,), (1,)), ((), ())), preferred_element_type=jnp.float32)
    rows, chunk = bias.shape
    return ((score * scale).reshape(tile, rows, chunk) + bias[None]).reshape(tile * rows, chunk)


def pair_kernel(
    rows_z, cols_x, group, spans, k_hbm, v_hbm, q_hbm, len_hbm, order_hbm, w_ref, v_ref, acc_ref, live_ref,
    q_ref, k_ref, own_w_ref, top_ref, bias_ref, len_ref, order_ref, q_sem, small_sem, *sems
):
    rows = q_ref.shape[0]
    half = rows_z * rows
    x = lax.rem(lax.axis_index("blk"), cols_x)
    own, other = (pl.ds(pl.multiple_of(side * half, half), half) for side in (x, 1 - x))
    q_copy = pltpu.make_async_copy(q_hbm.at[0], q_ref, q_sem)
    len_copy = pltpu.make_async_copy(len_hbm, len_ref, small_sem.at[0])
    order_copy = pltpu.make_async_copy(order_hbm, order_ref, small_sem.at[1])
    copies = (len_copy, order_copy, q_copy)
    tile = HEADS_PER_TILE if group % HEADS_PER_TILE == 0 else 1
    height = tile * rows
    tiles = group // tile

    def prepare():
        for copy in copies:
            copy.wait()
        row_pos = row_positions(order_ref, spans, rows)
        for n, side in enumerate((x, 1 - x)):
            key_pos = key_positions(order_ref, side * rows_z, (1, half), rows_z, cols_x, spans, rows)
            bias_ref[n] = mask(key_pos, row_pos)
        live_ref[...] = jnp.broadcast_to(jnp.where(row_pos < len_ref[0], 1.0, 0.0), live_ref.shape)

    def each_tile(visit):
        for h in range(k_ref.shape[1] // HEAD_WIDTH):

            def go(i, h=h):
                kept = pl.ds(pl.multiple_of((h * tiles + i) * height, height), height)
                visit(h * tiles + i, kept, slice(h * HEAD_WIDTH, (h + 1) * HEAD_WIDTH))

            pl.loop(0, tiles, unroll=True)(go)

    def own_keys():
        def visit(n, kept, cols):
            _, q = stacked_queries(q_ref, n * tile * HEAD_WIDTH, tile)
            score = scores(q, k_ref[own, cols], bias_ref[0], tile)
            top = jnp.max(score, axis=1, keepdims=True)
            own_w_ref[kept] = jnp.exp2(score - top).astype(jnp.bfloat16)
            top_ref[kept] = jnp.broadcast_to(top, (height, HEAD_WIDTH))

        each_tile(visit)

    arrived, drain = exchange(
        rows_z, cols_x, (k_hbm, v_hbm), (k_ref, v_ref), lambda: [copy.start() for copy in copies], prepare, own_keys,
        *sems
    )

    def own_values(n, kept, cols):
        acc_ref[kept] = jnp.dot(own_w_ref[kept], with_ones(v_ref[own, cols]), preferred_element_type=jnp.float32)

    each_tile(own_values)
    arrived(0)

    def other_keys(n, kept, cols):
        _, q = stacked_queries(q_ref, n * tile * HEAD_WIDTH, tile)
        score = scores(q, k_ref[other, cols], bias_ref[1], tile)
        best = top_ref[kept]
        top = jnp.maximum(best, jnp.max(score, axis=1, keepdims=True))
        wide_top = jnp.concatenate([top] * (half // HEAD_WIDTH), axis=1)
        w_ref[kept] = jnp.exp2(score - wide_top).astype(jnp.bfloat16)
        fade = jnp.exp2(best - top)
        acc_ref[kept] = acc_ref[kept] * jnp.concatenate([fade, fade], axis=1)

    each_tile(other_keys)
    arrived(1)
    drain()


def store_heads(o_ref, mixed, live, cols, tile):
    rows = live.shape[0]
    out = mixed[:, :HEAD_WIDTH] / mixed[:, HEAD_WIDTH:]
    for t in range(tile):
        o_ref[:, cols(t)] = jnp.where(live, out[t * rows : (t + 1) * rows], 0.0).astype(o_ref.dtype)


def with_ones(values):
    return jnp.concatenate([values, jnp.ones((values.shape[0], HEAD_WIDTH), values.dtype)], axis=1)


def in_parts(o_hbm, o_ref, out_sem, local_heads, group, tile, visit, unroll):
    tiles = group // tile
    per_part = tiles // OUT_PARTS
    wide = group * HEAD_WIDTH // OUT_PARTS
    copies = []
    for h in range(local_heads):
        for p in range(OUT_PARTS):
            pl.loop(p * per_part, (p + 1) * per_part, unroll=unroll)(lambda i, h=h: visit(h, i))
            at = pl.ds((h * OUT_PARTS + p) * wide, wide)
            copies.append(pltpu.make_async_copy(o_ref.at[:, at], o_hbm.at[0, :, at], out_sem.at[h, p]))
            copies[-1].start()
    for copy in copies:
        copy.wait()


def mix_kernel(cols_x, group, w_ref, v_ref, acc_ref, live_ref, o_hbm, o_ref, out_sem):
    tile = HEADS_PER_TILE if group % HEADS_PER_TILE == 0 else 1
    height = tile * o_ref.shape[0]
    half = w_ref.shape[1]
    side = 1 - lax.rem(lax.axis_index("blk"), cols_x)
    other = pl.ds(pl.multiple_of(side * half, half), half)
    live = live_ref[...] > 0.0

    def visit(h, i):
        first = (h * group + i * tile) * HEAD_WIDTH
        kept = pl.ds(pl.multiple_of((h * (group // tile) + i) * height, height), height)
        values = with_ones(v_ref[other, h * HEAD_WIDTH : (h + 1) * HEAD_WIDTH])
        mixed = acc_ref[kept] + jnp.dot(w_ref[kept], values, preferred_element_type=jnp.float32)

        def cols(t):
            return pl.ds(pl.multiple_of(first + t * HEAD_WIDTH, HEAD_WIDTH), HEAD_WIDTH)

        store_heads(o_ref, mixed, live, cols, tile)

    in_parts(o_hbm, o_ref, out_sem, v_ref.shape[1] // HEAD_WIDTH, group, tile, visit, True)


def attend_kernel(
    rows_z, cols_x, group, spans, q_hbm, k_ref, v_ref, len_hbm, order_hbm, o_hbm,
    q_ref, o_ref, bias_ref, len_ref, order_ref, q_sem, small_sem, out_sem
):
    q_copy = pltpu.make_async_copy(q_hbm.at[0], q_ref, q_sem)
    len_copy = pltpu.make_async_copy(len_hbm, len_ref, small_sem.at[0])
    order_copy = pltpu.make_async_copy(order_hbm, order_ref, small_sem.at[1])
    for copy in (len_copy, order_copy, q_copy):
        copy.start()
    rows = q_ref.shape[0]
    chunks, _, chunk = bias_ref.shape
    len_copy.wait()
    order_copy.wait()
    row_pos = row_positions(order_ref, spans, rows)

    def fill(c):
        first = c * (chunk // rows)
        bias_ref[c] = mask(key_positions(order_ref, first, (1, chunk), rows_z, cols_x, spans, rows), row_pos)

    pl.loop(0, chunks)(fill)
    live = row_pos < len_ref[0]
    q_copy.wait()
    tile = HEADS_PER_TILE if group % HEADS_PER_TILE == 0 else 1
    height = tile * rows

    def visit(h, i):
        cols = slice(h * HEAD_WIDTH, (h + 1) * HEAD_WIDTH)
        q_cols, q = stacked_queries(q_ref, (h * group + i * tile) * HEAD_WIDTH, tile)

        def step(c, state):
            best, mixed = state
            at = pl.ds(pl.multiple_of(c * chunk, chunk), chunk)
            score = scores(q, k_ref[at, cols], bias_ref[c], tile)
            top = jnp.maximum(best, jnp.max(score, axis=1, keepdims=True))
            weight = jnp.exp2(score - top).astype(jnp.bfloat16)
            fresh = jnp.dot(weight, with_ones(v_ref[at, cols]), preferred_element_type=jnp.float32)
            return top, mixed * jnp.exp2(best - top) + fresh

        init = (
            jnp.full((height, 1), NEG_FILL, jnp.float32),
            jnp.zeros((height, 2 * HEAD_WIDTH), jnp.float32),
        )
        _, mixed = lax.fori_loop(0, chunks, step, init)
        store_heads(o_ref, mixed, live, q_cols, tile)

    in_parts(o_hbm, o_ref, out_sem, k_ref.shape[1] // HEAD_WIDTH, group, tile, visit, False)


def solution(mesh):
    blocks = mesh.shape["blk"]
    cols_x = row_length(blocks)
    rows_z = blocks // cols_x
    dma = pltpu.SemaphoreType.DMA
    hbm = pl.BlockSpec(memory_space=pltpu.HBM)
    vmem = pl.BlockSpec(memory_space=pltpu.VMEM)

    def shards(queries, keys, values, prompt_length, span_order):
        _, rows, width = queries.shape
        kv_width = keys.shape[2]
        local_heads = kv_width // HEAD_WIDTH
        group = width // kv_width
        total = blocks * rows
        chunk = min(total, KEY_CHUNK)
        spans = span_order.shape[0] // blocks
        queries, keys, values, span_order = (
            pltpu.with_memory_space_constraint(a, pltpu.HBM) for a in (queries, keys, values, span_order)
        )
        exchange_sems = [
            dma((2,)),
            pltpu.SemaphoreType.REGULAR((rows_z,)),
            pltpu.SemaphoreType.REGULAR((cols_x,)),
            dma((2,)),
            dma((2,)),
            dma((rows_z, 2)),
            dma((2,)),
        ]
        small = [pltpu.SMEM(prompt_length.shape, jnp.int32), pltpu.SMEM(span_order.shape, jnp.int32)]
        talk = pltpu.CompilerParams(collective_id=0, has_side_effects=True, vmem_limit_bytes=VMEM_LIMIT)
        quiet = pltpu.CompilerParams(vmem_limit_bytes=VMEM_LIMIT)
        out_shape = jax.ShapeDtypeStruct(queries.shape, queries.dtype)
        out_sems = dma((local_heads, OUT_PARTS))
        gathered = pltpu.VMEM((total, kv_width), keys.dtype)
        bias = pltpu.VMEM((total // chunk, rows, chunk), jnp.float32)
        wide = pltpu.VMEM((rows, width), queries.dtype)
        if chunk == total and cols_x == 2:
            queue = local_heads * group * rows
            half = total // 2
            parts = pl.pallas_call(
                functools.partial(pair_kernel, rows_z, cols_x, group, spans),
                out_shape=[
                    pltpu.VMEM((queue, half), jnp.bfloat16),
                    gathered,
                    pltpu.VMEM((queue, 2 * HEAD_WIDTH), jnp.float32),
                    pltpu.VMEM((rows, HEAD_WIDTH), jnp.float32),
                ],
                in_specs=[hbm] * 5,
                out_specs=[vmem] * 4,
                scratch_shapes=[
                    wide,
                    gathered,
                    pltpu.VMEM((queue, half), jnp.bfloat16),
                    pltpu.VMEM((queue, HEAD_WIDTH), jnp.float32),
                    pltpu.VMEM((2, rows, half), jnp.float32),
                    *small,
                    dma,
                    dma((2,)),
                    *exchange_sems,
                ],
                compiler_params=talk,
            )(keys, values, queries, prompt_length, span_order)
            return pl.pallas_call(
                functools.partial(mix_kernel, cols_x, group),
                out_shape=out_shape,
                in_specs=[vmem] * 4,
                out_specs=hbm,
                scratch_shapes=[wide, out_sems],
                compiler_params=quiet,
            )(*parts)
        k_all, v_all = pl.pallas_call(
            functools.partial(gather_kernel, rows_z, cols_x),
            out_shape=[gathered] * 2,
            in_specs=[hbm] * 2,
            out_specs=[vmem] * 2,
            scratch_shapes=exchange_sems,
            compiler_params=talk,
        )(keys, values)
        return pl.pallas_call(
            functools.partial(attend_kernel, rows_z, cols_x, group, spans),
            out_shape=out_shape,
            in_specs=[hbm, vmem, vmem, hbm, hbm],
            out_specs=hbm,
            scratch_shapes=[wide, wide, bias, *small, dma, dma((2,)), out_sems],
            compiler_params=quiet,
        )(queries, k_all, v_all, prompt_length, span_order)

    spec = P("rep", "blk", "head")
    return jax.shard_map(
        shards, mesh=mesh, in_specs=(spec, spec, spec, P("rep"), P("rep")), out_specs=spec, check_vma=False
    )
```

```python
import functools
import math

import jax
import jax.numpy as jnp
from jax import lax
from jax.experimental import pallas as pl
from jax.experimental.pallas import tpu as pltpu
from jax.sharding import PartitionSpec as P

HEAD_WIDTH = 128
NEG_FILL = -1e30
HEADS_PER_TILE = 2
KEY_CHUNK = 512
OUT_PARTS = 2
VMEM_LIMIT = 40 * 1024 * 1024
MESH = pl.DeviceIdType.MESH


def row_length(blocks):
    return max(d for d in range(1, math.isqrt(blocks) + 1) if blocks % d == 0)


def row_positions(order_ref, spans, rows):
    span = rows // spans
    index = lax.broadcasted_iota(jnp.int32, (rows, 1), 0)
    position = jnp.zeros((rows, 1), jnp.int32)
    for t in range(spans):
        first = order_ref[lax.axis_index("blk") * spans + t] * span
        position = jnp.where(index // span == t, first + index % span, position)
    return position


def key_positions(order_ref, first_block, shape, rows_z, cols_x, spans, rows):
    span = rows // spans
    index = lax.broadcasted_iota(jnp.int32, shape, 1)
    position = jnp.zeros(shape, jnp.int32)
    for t in range(shape[1] // span):
        slot = first_block + t // spans
        block = lax.rem(slot, rows_z) * cols_x + lax.div(slot, rows_z)
        first = order_ref[block * spans + t % spans] * span
        position = jnp.where(index // span == t, first + index % span, position)
    return position


def mask(key_pos, row_pos):
    return jnp.where(key_pos <= row_pos, 0.0, NEG_FILL)


def exchange(rows_z, cols_x, sources, refs, meanwhile, prepare, own_keys, own_sem, ready_z, ready_x, z_send, x_send, z_recv, x_recv):
    rows = sources[0].shape[1]
    me = lax.axis_index("blk")
    z, x = lax.div(me, cols_x), lax.rem(me, cols_x)
    even = lax.rem(z, 2) == 0
    first = lax.axis_index("head") == 0
    near = range(1, rows_z)
    far = range(rows_z - 1, 0, -1)
    own = pl.ds((x * rows_z + z) * rows, rows)
    loads = [pltpu.make_async_copy(sources[u].at[0], refs[u].at[own], own_sem.at[u]) for u in range(2)]
    for load in loads:
        load.start()
    meanwhile()

    def send(source, u, row, to_row, to_col, send_sem, recv_sem):
        at = pl.ds((x * rows_z + row) * rows, rows)
        return pltpu.make_async_remote_copy(
            src_ref=refs[u].at[at] if source is None else source,
            dst_ref=refs[u].at[at],
            send_sem=send_sem,
            recv_sem=recv_sem,
            device_id={"blk": to_row * cols_x + to_col},
            device_id_type=MESH,
        )

    def z_copy(row, to_row, u, source=None):
        return send(source, u, row, to_row, x, z_send.at[u], z_recv.at[row, u])

    def x_copy(row, col, u):
        return send(None, u, row, z, col, x_send.at[u], x_recv.at[u])

    def above(d, visit):
        pl.when(z + d < rows_z)(lambda: visit(z + d))

    def below(d, visit):
        pl.when(z >= d)(lambda: visit(z - d))

    def right(visit):
        for e in range(1, cols_x):
            pl.when(x + e < cols_x)(lambda e=e: visit(x + e))

    def left(visit):
        for e in range(1, cols_x):
            pl.when(x >= e)(lambda e=e: visit(x - e))

    def spread(row, u):
        for e in range(1, cols_x):
            x_copy(row, lax.rem(x + e, cols_x), u).start()

    def signal(sem, row, col):
        pl.semaphore_signal(sem, inc=1, device_id={"blk": row * cols_x + col}, device_id_type=MESH)

    barrier = pltpu.get_barrier_semaphore()
    for d in near:
        above(d, lambda row: signal(barrier, row, x))
    right(lambda col: signal(barrier, z, col))
    pl.when(z + x > 0)(lambda: pl.semaphore_wait(barrier, z + x))
    for d in far:
        below(d, lambda row: signal(ready_z.at[z], row, x))
    left(lambda col: signal(ready_x.at[x], z, col))

    def straight(u):
        return first & (u == 1)

    def send_below(u):
        for d in far:
            go = functools.partial(below, d, lambda row: z_copy(z, row, u, sources[u].at[0]).start())
            if d == 2:
                pl.when(even | straight(u))(go)
            else:
                go()

    def send_above(d, *which):
        for u in which:
            go = functools.partial(above, d, lambda row, u=u: z_copy(z, row, u, sources[u].at[0]).start())
            if d == 2:
                pl.when(even)(go)
            elif d == 3:
                pl.when(straight(u))(go)
            else:
                go()

    def answered(d):
        above(d, lambda row: pl.semaphore_wait(ready_z.at[row], 1))

    def relay_from_below(d, u):
        def take(row):
            z_copy(row, z, u).wait_recv()
            if d == 1:
                pl.when(even & (z + 1 < rows_z))(lambda: z_copy(row, z + 1, u).start())
            if d == 2:
                pl.when((z + 1 < rows_z) & ~straight(u))(lambda: z_copy(row, z + 1, u).start())
            spread(row, u)

        below(d, take)

    def relay_from_above(d, u):
        def take(row):
            z_copy(row, z, u).wait_recv()
            spread(row, u)
            if d == 1:
                pl.when(even & (z >= 1) & ~straight(u))(lambda: z_copy(row, z - 1, u).start())

        above(d, take)

    def relay(d, u):
        relay_from_below(d, u)
        relay_from_above(d, u)

    def send_left(u):
        loads[u].wait()
        left(lambda col: x_copy(z, col, u).start())

    def send_right(*which):
        right(lambda col: pl.semaphore_wait(ready_x.at[col], 1))
        for u in which:
            right(lambda col: x_copy(z, col, u).start())

    def eager():
        for u in range(2):
            send_below(u)
            send_left(u)
        send_right(0, 1)
        for d in near:
            answered(d)
            send_above(d, 0, 1)

    def patient():
        send_below(0)
        send_left(0)
        send_left(1)
        send_right(0, 1)
        for d in near:
            answered(d)
            send_above(d, 0)

    pl.when(first)(eager)
    pl.when(~first)(patient)
    prepare()
    lowest = first & (z == 0)
    inner = first & (z > 0) & (z < rows_z - 1)

    def values_now():
        send_below(1)
        for d in near:
            send_above(d, 1)

    for d in near:
        relay(d, 0)
        if d == 1:
            pl.when(lowest)(lambda: relay_from_above(1, 1))
            pl.when(inner)(lambda: relay_from_below(1, 1))
            pl.when(~first)(values_now)
    pl.when(~inner)(lambda: relay_from_below(1, 1))
    for d in near[1:]:
        relay_from_below(d, 1)
    pl.when(~lowest)(lambda: relay_from_above(1, 1))
    for d in near[1:]:
        relay_from_above(d, 1)
    own_keys()

    def many(u, count, sem):
        at = pl.ds(0, count * rows)
        return pltpu.make_async_copy(refs[u].at[at], refs[u].at[at], sem)

    along_x = (cols_x - 1) * rows_z

    def arrived(u):
        many(u, along_x, x_recv.at[u]).wait()

    def sent_along_z(row, detours):
        odd, inside = row % 2 == 1, 0 < row < rows_z - 1
        count = rows_z - 1 - (odd and row + 2 < rows_z) + (not odd and inside)
        if detours:
            count += (row >= 2 and row + 1 < rows_z) - (row + 3 < rows_z)
            count += (not odd and inside) - (odd and row >= 2)
        return count

    def drain():
        for u in range(2):
            many(u, along_x, x_send.at[u]).wait()
            for row in range(rows_z):
                for detours in (True, False):
                    here = (z == row) & (straight(u) != detours)
                    count = sent_along_z(row, detours)
                    pl.when(here)(lambda u=u, count=count: many(u, count, z_send.at[u]).wait())

    return arrived, drain


def gather_kernel(rows_z, cols_x, k_hbm, v_hbm, k_ref, v_ref, *sems):
    arrived, drain = exchange(rows_z, cols_x, (k_hbm, v_hbm), (k_ref, v_ref), *[lambda: None] * 3, *sems)
    arrived(0)
    arrived(1)
    drain()


def stacked_queries(q_ref, first, tile):
    def cols(t):
        return pl.ds(pl.multiple_of(first + t * HEAD_WIDTH, HEAD_WIDTH), HEAD_WIDTH)

    return cols, jnp.concatenate([q_ref[:, cols(t)] for t in range(tile)], axis=0)


def scores(q, keys, bias, tile):
    scale = HEAD_WIDTH ** (-0.5) * math.log2(math.e)
    score = lax.dot_general(q, keys, (((1,), (1,)), ((), ())), preferred_element_type=jnp.float32)
    rows, chunk = bias.shape
    return ((score * scale).reshape(tile, rows, chunk) + bias[None]).reshape(tile * rows, chunk)


def pair_kernel(
    rows_z, cols_x, group, spans, k_hbm, v_hbm, q_hbm, len_hbm, order_hbm, w_ref, v_ref, acc_ref, live_ref,
    q_ref, k_ref, own_w_ref, top_ref, bias_ref, len_ref, order_ref, q_sem, small_sem, *sems
):
    rows = q_ref.shape[0]
    half = rows_z * rows
    x = lax.rem(lax.axis_index("blk"), cols_x)
    own, other = (pl.ds(pl.multiple_of(side * half, half), half) for side in (x, 1 - x))
    q_copy = pltpu.make_async_copy(q_hbm.at[0], q_ref, q_sem)
    len_copy = pltpu.make_async_copy(len_hbm, len_ref, small_sem.at[0])
    order_copy = pltpu.make_async_copy(order_hbm, order_ref, small_sem.at[1])
    copies = (len_copy, order_copy, q_copy)
    tile = HEADS_PER_TILE if group % HEADS_PER_TILE == 0 else 1
    height = tile * rows
    tiles = group // tile

    def prepare():
        for copy in copies:
            copy.wait()
        row_pos = row_positions(order_ref, spans, rows)
        for n, side in enumerate((x, 1 - x)):
            key_pos = key_positions(order_ref, side * rows_z, (1, half), rows_z, cols_x, spans, rows)
            bias_ref[n] = mask(key_pos, row_pos)
        live_ref[...] = jnp.broadcast_to(jnp.where(row_pos < len_ref[0], 1.0, 0.0), live_ref.shape)

    def each_tile(visit):
        for h in range(k_ref.shape[1] // HEAD_WIDTH):

            def go(i, h=h):
                kept = pl.ds(pl.multiple_of((h * tiles + i) * height, height), height)
                visit(h * tiles + i, kept, slice(h * HEAD_WIDTH, (h + 1) * HEAD_WIDTH))

            pl.loop(0, tiles, unroll=True)(go)

    def own_keys():
        def visit(n, kept, cols):
            _, q = stacked_queries(q_ref, n * tile * HEAD_WIDTH, tile)
            score = scores(q, k_ref[own, cols], bias_ref[0], tile)
            top = jnp.max(score, axis=1, keepdims=True)
            own_w_ref[kept] = jnp.exp2(score - top).astype(jnp.bfloat16)
            top_ref[kept] = jnp.broadcast_to(top, (height, HEAD_WIDTH))

        each_tile(visit)

    arrived, drain = exchange(
        rows_z, cols_x, (k_hbm, v_hbm), (k_ref, v_ref), lambda: [copy.start() for copy in copies], prepare, own_keys,
        *sems
    )

    def own_values(n, kept, cols):
        acc_ref[kept] = jnp.dot(own_w_ref[kept], with_ones(v_ref[own, cols]), preferred_element_type=jnp.float32)

    each_tile(own_values)
    arrived(0)

    def other_keys(n, kept, cols):
        _, q = stacked_queries(q_ref, n * tile * HEAD_WIDTH, tile)
        score = scores(q, k_ref[other, cols], bias_ref[1], tile)
        best = top_ref[kept]
        top = jnp.maximum(best, jnp.max(score, axis=1, keepdims=True))
        wide_top = jnp.concatenate([top] * (half // HEAD_WIDTH), axis=1)
        w_ref[kept] = jnp.exp2(score - wide_top).astype(jnp.bfloat16)
        fade = jnp.exp2(best - top)
        acc_ref[kept] = acc_ref[kept] * jnp.concatenate([fade, fade], axis=1)

    each_tile(other_keys)
    arrived(1)
    drain()


def store_heads(o_ref, mixed, live, cols, tile):
    rows = live.shape[0]
    out = mixed[:, :HEAD_WIDTH] / mixed[:, HEAD_WIDTH:]
    for t in range(tile):
        o_ref[:, cols(t)] = jnp.where(live, out[t * rows : (t + 1) * rows], 0.0).astype(o_ref.dtype)


def with_ones(values):
    return jnp.concatenate([values, jnp.ones((values.shape[0], HEAD_WIDTH), values.dtype)], axis=1)


def in_parts(o_hbm, o_ref, out_sem, local_heads, group, tile, visit, unroll):
    tiles = group // tile
    per_part = tiles // OUT_PARTS
    wide = group * HEAD_WIDTH // OUT_PARTS
    copies = []
    for h in range(local_heads):
        for p in range(OUT_PARTS):
            pl.loop(p * per_part, (p + 1) * per_part, unroll=unroll)(lambda i, h=h: visit(h, i))
            at = pl.ds((h * OUT_PARTS + p) * wide, wide)
            copies.append(pltpu.make_async_copy(o_ref.at[:, at], o_hbm.at[0, :, at], out_sem.at[h, p]))
            copies[-1].start()
    for copy in copies:
        copy.wait()


def mix_kernel(cols_x, group, w_ref, v_ref, acc_ref, live_ref, o_hbm, o_ref, out_sem):
    tile = HEADS_PER_TILE if group % HEADS_PER_TILE == 0 else 1
    height = tile * o_ref.shape[0]
    half = w_ref.shape[1]
    side = 1 - lax.rem(lax.axis_index("blk"), cols_x)
    other = pl.ds(pl.multiple_of(side * half, half), half)
    live = live_ref[...] > 0.0

    def visit(h, i):
        first = (h * group + i * tile) * HEAD_WIDTH
        kept = pl.ds(pl.multiple_of((h * (group // tile) + i) * height, height), height)
        values = with_ones(v_ref[other, h * HEAD_WIDTH : (h + 1) * HEAD_WIDTH])
        mixed = acc_ref[kept] + jnp.dot(w_ref[kept], values, preferred_element_type=jnp.float32)

        def cols(t):
            return pl.ds(pl.multiple_of(first + t * HEAD_WIDTH, HEAD_WIDTH), HEAD_WIDTH)

        store_heads(o_ref, mixed, live, cols, tile)

    in_parts(o_hbm, o_ref, out_sem, v_ref.shape[1] // HEAD_WIDTH, group, tile, visit, True)


def attend_kernel(
    rows_z, cols_x, group, spans, q_hbm, k_ref, v_ref, len_hbm, order_hbm, o_hbm,
    q_ref, o_ref, bias_ref, len_ref, order_ref, q_sem, small_sem, out_sem
):
    q_copy = pltpu.make_async_copy(q_hbm.at[0], q_ref, q_sem)
    len_copy = pltpu.make_async_copy(len_hbm, len_ref, small_sem.at[0])
    order_copy = pltpu.make_async_copy(order_hbm, order_ref, small_sem.at[1])
    for copy in (len_copy, order_copy, q_copy):
        copy.start()
    rows = q_ref.shape[0]
    chunks, _, chunk = bias_ref.shape
    len_copy.wait()
    order_copy.wait()
    row_pos = row_positions(order_ref, spans, rows)

    def fill(c):
        first = c * (chunk // rows)
        bias_ref[c] = mask(key_positions(order_ref, first, (1, chunk), rows_z, cols_x, spans, rows), row_pos)

    pl.loop(0, chunks)(fill)
    live = row_pos < len_ref[0]
    q_copy.wait()
    tile = HEADS_PER_TILE if group % HEADS_PER_TILE == 0 else 1
    height = tile * rows

    def visit(h, i):
        cols = slice(h * HEAD_WIDTH, (h + 1) * HEAD_WIDTH)
        q_cols, q = stacked_queries(q_ref, (h * group + i * tile) * HEAD_WIDTH, tile)

        def step(c, state):
            best, mixed = state
            at = pl.ds(pl.multiple_of(c * chunk, chunk), chunk)
            score = scores(q, k_ref[at, cols], bias_ref[c], tile)
            top = jnp.maximum(best, jnp.max(score, axis=1, keepdims=True))
            weight = jnp.exp2(score - top).astype(jnp.bfloat16)
            fresh = jnp.dot(weight, with_ones(v_ref[at, cols]), preferred_element_type=jnp.float32)
            return top, mixed * jnp.exp2(best - top) + fresh

        init = (
            jnp.full((height, 1), NEG_FILL, jnp.float32),
            jnp.zeros((height, 2 * HEAD_WIDTH), jnp.float32),
        )
        _, mixed = lax.fori_loop(0, chunks, step, init)
        store_heads(o_ref, mixed, live, q_cols, tile)

    in_parts(o_hbm, o_ref, out_sem, k_ref.shape[1] // HEAD_WIDTH, group, tile, visit, False)


def solution(mesh):
    blocks = mesh.shape["blk"]
    cols_x = row_length(blocks)
    rows_z = blocks // cols_x
    dma = pltpu.SemaphoreType.DMA
    hbm = pl.BlockSpec(memory_space=pltpu.HBM)
    vmem = pl.BlockSpec(memory_space=pltpu.VMEM)

    def shards(queries, keys, values, prompt_length, span_order):
        _, rows, width = queries.shape
        kv_width = keys.shape[2]
        local_heads = kv_width // HEAD_WIDTH
        group = width // kv_width
        total = blocks * rows
        chunk = min(total, KEY_CHUNK)
        spans = span_order.shape[0] // blocks
        queries, keys, values, span_order = (
            pltpu.with_memory_space_constraint(a, pltpu.HBM) for a in (queries, keys, values, span_order)
        )
        exchange_sems = [
            dma((2,)),
            pltpu.SemaphoreType.REGULAR((rows_z,)),
            pltpu.SemaphoreType.REGULAR((cols_x,)),
            dma((2,)),
            dma((2,)),
            dma((rows_z, 2)),
            dma((2,)),
        ]
        small = [pltpu.SMEM(prompt_length.shape, jnp.int32), pltpu.SMEM(span_order.shape, jnp.int32)]
        talk = pltpu.CompilerParams(collective_id=0, has_side_effects=True, vmem_limit_bytes=VMEM_LIMIT)
        quiet = pltpu.CompilerParams(vmem_limit_bytes=VMEM_LIMIT)
        out_shape = jax.ShapeDtypeStruct(queries.shape, queries.dtype)
        out_sems = dma((local_heads, OUT_PARTS))
        gathered = pltpu.VMEM((total, kv_width), keys.dtype)
        bias = pltpu.VMEM((total // chunk, rows, chunk), jnp.float32)
        wide = pltpu.VMEM((rows, width), queries.dtype)
        if chunk == total and cols_x == 2:
            queue = local_heads * group * rows
            half = total // 2
            parts = pl.pallas_call(
                functools.partial(pair_kernel, rows_z, cols_x, group, spans),
                out_shape=[
                    pltpu.VMEM((queue, half), jnp.bfloat16),
                    gathered,
                    pltpu.VMEM((queue, 2 * HEAD_WIDTH), jnp.float32),
                    pltpu.VMEM((rows, HEAD_WIDTH), jnp.float32),
                ],
                in_specs=[hbm] * 5,
                out_specs=[vmem] * 4,
                scratch_shapes=[
                    wide,
                    gathered,
                    pltpu.VMEM((queue, half), jnp.bfloat16),
                    pltpu.VMEM((queue, HEAD_WIDTH), jnp.float32),
                    pltpu.VMEM((2, rows, half), jnp.float32),
                    *small,
                    dma,
                    dma((2,)),
                    *exchange_sems,
                ],
                compiler_params=talk,
            )(keys, values, queries, prompt_length, span_order)
            return pl.pallas_call(
                functools.partial(mix_kernel, cols_x, group),
                out_shape=out_shape,
                in_specs=[vmem] * 4,
                out_specs=hbm,
                scratch_shapes=[wide, out_sems],
                compiler_params=quiet,
            )(*parts)
        k_all, v_all = pl.pallas_call(
            functools.partial(gather_kernel, rows_z, cols_x),
            out_shape=[gathered] * 2,
            in_specs=[hbm] * 2,
            out_specs=[vmem] * 2,
            scratch_shapes=exchange_sems,
            compiler_params=talk,
        )(keys, values)
        return pl.pallas_call(
            functools.partial(attend_kernel, rows_z, cols_x, group, spans),
            out_shape=out_shape,
            in_specs=[hbm, vmem, vmem, hbm, hbm],
            out_specs=hbm,
            scratch_shapes=[wide, wide, bias, *small, dma, dma((2,)), out_sems],
            compiler_params=quiet,
        )(queries, k_all, v_all, prompt_length, span_order)

    spec = P("rep", "blk", "head")
    return jax.shard_map(
        shards, mesh=mesh, in_specs=(spec, spec, spec, P("rep"), P("rep")), out_specs=spec, check_vma=False
    )
```

```python
import functools
import math

import jax
import jax.numpy as jnp
from jax import lax
from jax.experimental import pallas as pl
from jax.experimental.pallas import tpu as pltpu
from jax.sharding import PartitionSpec as P

HEAD_WIDTH = 128
NEG_FILL = -1e30
HEADS_PER_TILE = 2
KEY_CHUNK = 512
OUT_PARTS = 2
VMEM_LIMIT = 40 * 1024 * 1024
MESH = pl.DeviceIdType.MESH


def row_length(blocks):
    return max(d for d in range(1, math.isqrt(blocks) + 1) if blocks % d == 0)


def row_positions(order_ref, spans, rows):
    span = rows // spans
    index = lax.broadcasted_iota(jnp.int32, (rows, 1), 0)
    position = jnp.zeros((rows, 1), jnp.int32)
    for t in range(spans):
        first = order_ref[lax.axis_index("blk") * spans + t] * span
        position = jnp.where(index // span == t, first + index % span, position)
    return position


def key_positions(order_ref, first_block, shape, rows_z, cols_x, spans, rows):
    span = rows // spans
    index = lax.broadcasted_iota(jnp.int32, shape, 1)
    position = jnp.zeros(shape, jnp.int32)
    for t in range(shape[1] // span):
        slot = first_block + t // spans
        block = lax.rem(slot, rows_z) * cols_x + lax.div(slot, rows_z)
        first = order_ref[block * spans + t % spans] * span
        position = jnp.where(index // span == t, first + index % span, position)
    return position


def mask(key_pos, row_pos):
    return jnp.where(key_pos <= row_pos, 0.0, NEG_FILL)


def exchange(rows_z, cols_x, sources, refs, meanwhile, prepare, own_keys, own_sem, ready_z, ready_x, z_send, x_send, z_recv, x_recv):
    rows = sources[0].shape[1]
    me = lax.axis_index("blk")
    z, x = lax.div(me, cols_x), lax.rem(me, cols_x)
    even = lax.rem(z, 2) == 0
    first = lax.axis_index("head") == 0
    near = range(1, rows_z)
    far = range(rows_z - 1, 0, -1)
    own = pl.ds((x * rows_z + z) * rows, rows)
    loads = [pltpu.make_async_copy(sources[u].at[0], refs[u].at[own], own_sem.at[u]) for u in range(2)]
    for load in loads:
        load.start()
    meanwhile()

    def send(source, u, row, to_row, to_col, send_sem, recv_sem):
        at = pl.ds((x * rows_z + row) * rows, rows)
        return pltpu.make_async_remote_copy(
            src_ref=refs[u].at[at] if source is None else source,
            dst_ref=refs[u].at[at],
            send_sem=send_sem,
            recv_sem=recv_sem,
            device_id={"blk": to_row * cols_x + to_col},
            device_id_type=MESH,
        )

    def z_copy(row, to_row, u, source=None):
        return send(source, u, row, to_row, x, z_send.at[u], z_recv.at[row, u])

    def x_copy(row, col, u):
        return send(None, u, row, z, col, x_send.at[u], x_recv.at[u])

    def above(d, visit):
        pl.when(z + d < rows_z)(lambda: visit(z + d))

    def below(d, visit):
        pl.when(z >= d)(lambda: visit(z - d))

    def right(visit):
        for e in range(1, cols_x):
            pl.when(x + e < cols_x)(lambda e=e: visit(x + e))

    def left(visit):
        for e in range(1, cols_x):
            pl.when(x >= e)(lambda e=e: visit(x - e))

    def spread(row, u):
        for e in range(1, cols_x):
            x_copy(row, lax.rem(x + e, cols_x), u).start()

    def signal(sem, row, col):
        pl.semaphore_signal(sem, inc=1, device_id={"blk": row * cols_x + col}, device_id_type=MESH)

    barrier = pltpu.get_barrier_semaphore()
    for d in near:
        above(d, lambda row: signal(barrier, row, x))
    right(lambda col: signal(barrier, z, col))
    pl.when(z + x > 0)(lambda: pl.semaphore_wait(barrier, z + x))
    for d in far:
        below(d, lambda row: signal(ready_z.at[z], row, x))
    left(lambda col: signal(ready_x.at[x], z, col))

    def straight(u):
        return first & (u == 1)

    def send_below(u):
        for d in far:
            go = functools.partial(below, d, lambda row: z_copy(z, row, u, sources[u].at[0]).start())
            if d == 2:
                pl.when(even | straight(u))(go)
            else:
                go()

    def send_above(d, *which):
        for u in which:
            go = functools.partial(above, d, lambda row, u=u: z_copy(z, row, u, sources[u].at[0]).start())
            if d == 2:
                pl.when(even)(go)
            elif d == 3:
                pl.when(straight(u))(go)
            else:
                go()

    def answered(d):
        above(d, lambda row: pl.semaphore_wait(ready_z.at[row], 1))

    def relay_from_below(d, u):
        def take(row):
            z_copy(row, z, u).wait_recv()
            if d == 1:
                pl.when(even & (z + 1 < rows_z))(lambda: z_copy(row, z + 1, u).start())
            if d == 2:
                pl.when((z + 1 < rows_z) & ~straight(u))(lambda: z_copy(row, z + 1, u).start())
            spread(row, u)

        below(d, take)

    def relay_from_above(d, u):
        def take(row):
            z_copy(row, z, u).wait_recv()
            spread(row, u)
            if d == 1:
                pl.when(even & (z >= 1) & ~straight(u))(lambda: z_copy(row, z - 1, u).start())

        above(d, take)

    def relay(d, u):
        relay_from_below(d, u)
        relay_from_above(d, u)

    def send_left(u):
        loads[u].wait()
        left(lambda col: x_copy(z, col, u).start())

    def send_right(*which):
        right(lambda col: pl.semaphore_wait(ready_x.at[col], 1))
        for u in which:
            right(lambda col: x_copy(z, col, u).start())

    def eager():
        for u in range(2):
            send_below(u)
            send_left(u)
        send_right(0, 1)
        for d in near:
            answered(d)
            send_above(d, 0, 1)

    def patient():
        send_below(0)
        send_left(0)
        send_left(1)
        send_right(0, 1)
        for d in near:
            answered(d)
            send_above(d, 0)

    pl.when(first)(eager)
    pl.when(~first)(patient)
    prepare()
    lowest = first & (z == 0)
    upper = first & (z > 0)

    def values_now():
        send_below(1)
        for d in near:
            send_above(d, 1)

    for d in near:
        relay(d, 0)
        if d == 1:
            pl.when(lowest)(lambda: relay_from_above(1, 1))
            pl.when(upper)(lambda: relay_from_below(1, 1))
            pl.when(~first)(values_now)
    pl.when(~upper)(lambda: relay_from_below(1, 1))
    for d in near[1:]:
        relay_from_below(d, 1)
    pl.when(~lowest)(lambda: relay_from_above(1, 1))
    for d in near[1:]:
        relay_from_above(d, 1)
    own_keys()

    def many(u, count, sem):
        at = pl.ds(0, count * rows)
        return pltpu.make_async_copy(refs[u].at[at], refs[u].at[at], sem)

    along_x = (cols_x - 1) * rows_z

    def arrived(u):
        many(u, along_x, x_recv.at[u]).wait()

    def sent_along_z(row, detours):
        odd, inside = row % 2 == 1, 0 < row < rows_z - 1
        count = rows_z - 1 - (odd and row + 2 < rows_z) + (not odd and inside)
        if detours:
            count += (row >= 2 and row + 1 < rows_z) - (row + 3 < rows_z)
            count += (not odd and inside) - (odd and row >= 2)
        return count

    def drain():
        for u in range(2):
            many(u, along_x, x_send.at[u]).wait()
            for row in range(rows_z):
                for detours in (True, False):
                    here = (z == row) & (straight(u) != detours)
                    count = sent_along_z(row, detours)
                    pl.when(here)(lambda u=u, count=count: many(u, count, z_send.at[u]).wait())

    return arrived, drain


def gather_kernel(rows_z, cols_x, k_hbm, v_hbm, k_ref, v_ref, *sems):
    arrived, drain = exchange(rows_z, cols_x, (k_hbm, v_hbm), (k_ref, v_ref), *[lambda: None] * 3, *sems)
    arrived(0)
    arrived(1)
    drain()


def stacked_queries(q_ref, first, tile):
    def cols(t):
        return pl.ds(pl.multiple_of(first + t * HEAD_WIDTH, HEAD_WIDTH), HEAD_WIDTH)

    return cols, jnp.concatenate([q_ref[:, cols(t)] for t in range(tile)], axis=0)


def scores(q, keys, bias, tile):
    scale = HEAD_WIDTH ** (-0.5) * math.log2(math.e)
    score = lax.dot_general(q, keys, (((1,), (1,)), ((), ())), preferred_element_type=jnp.float32)
    rows, chunk = bias.shape
    return ((score * scale).reshape(tile, rows, chunk) + bias[None]).reshape(tile * rows, chunk)


def pair_kernel(
    rows_z, cols_x, group, spans, k_hbm, v_hbm, q_hbm, len_hbm, order_hbm, w_ref, v_ref, acc_ref, live_ref,
    q_ref, k_ref, own_w_ref, top_ref, bias_ref, len_ref, order_ref, q_sem, small_sem, *sems
):
    rows = q_ref.shape[0]
    half = rows_z * rows
    x = lax.rem(lax.axis_index("blk"), cols_x)
    own, other = (pl.ds(pl.multiple_of(side * half, half), half) for side in (x, 1 - x))
    q_copy = pltpu.make_async_copy(q_hbm.at[0], q_ref, q_sem)
    len_copy = pltpu.make_async_copy(len_hbm, len_ref, small_sem.at[0])
    order_copy = pltpu.make_async_copy(order_hbm, order_ref, small_sem.at[1])
    copies = (len_copy, order_copy, q_copy)
    tile = HEADS_PER_TILE if group % HEADS_PER_TILE == 0 else 1
    height = tile * rows
    tiles = group // tile

    def prepare():
        for copy in copies:
            copy.wait()
        row_pos = row_positions(order_ref, spans, rows)
        for n, side in enumerate((x, 1 - x)):
            key_pos = key_positions(order_ref, side * rows_z, (1, half), rows_z, cols_x, spans, rows)
            bias_ref[n] = mask(key_pos, row_pos)
        live_ref[...] = jnp.broadcast_to(jnp.where(row_pos < len_ref[0], 1.0, 0.0), live_ref.shape)

    def each_tile(visit):
        for h in range(k_ref.shape[1] // HEAD_WIDTH):

            def go(i, h=h):
                kept = pl.ds(pl.multiple_of((h * tiles + i) * height, height), height)
                visit(h * tiles + i, kept, slice(h * HEAD_WIDTH, (h + 1) * HEAD_WIDTH))

            pl.loop(0, tiles, unroll=True)(go)

    def own_keys():
        def visit(n, kept, cols):
            _, q = stacked_queries(q_ref, n * tile * HEAD_WIDTH, tile)
            score = scores(q, k_ref[own, cols], bias_ref[0], tile)
            top = jnp.max(score, axis=1, keepdims=True)
            own_w_ref[kept] = jnp.exp2(score - top).astype(jnp.bfloat16)
            top_ref[kept] = jnp.broadcast_to(top, (height, HEAD_WIDTH))

        each_tile(visit)

    arrived, drain = exchange(
        rows_z, cols_x, (k_hbm, v_hbm), (k_ref, v_ref), lambda: [copy.start() for copy in copies], prepare, own_keys,
        *sems
    )

    def own_values(n, kept, cols):
        acc_ref[kept] = jnp.dot(own_w_ref[kept], with_ones(v_ref[own, cols]), preferred_element_type=jnp.float32)

    each_tile(own_values)
    arrived(0)

    def other_keys(n, kept, cols):
        _, q = stacked_queries(q_ref, n * tile * HEAD_WIDTH, tile)
        score = scores(q, k_ref[other, cols], bias_ref[1], tile)
        best = top_ref[kept]
        top = jnp.maximum(best, jnp.max(score, axis=1, keepdims=True))
        wide_top = jnp.concatenate([top] * (half // HEAD_WIDTH), axis=1)
        w_ref[kept] = jnp.exp2(score - wide_top).astype(jnp.bfloat16)
        fade = jnp.exp2(best - top)
        acc_ref[kept] = acc_ref[kept] * jnp.concatenate([fade, fade], axis=1)

    each_tile(other_keys)
    arrived(1)
    drain()


def store_heads(o_ref, mixed, live, cols, tile):
    rows = live.shape[0]
    out = mixed[:, :HEAD_WIDTH] / mixed[:, HEAD_WIDTH:]
    for t in range(tile):
        o_ref[:, cols(t)] = jnp.where(live, out[t * rows : (t + 1) * rows], 0.0).astype(o_ref.dtype)


def with_ones(values):
    return jnp.concatenate([values, jnp.ones((values.shape[0], HEAD_WIDTH), values.dtype)], axis=1)


def in_parts(o_hbm, o_ref, out_sem, local_heads, group, tile, visit, unroll):
    tiles = group // tile
    per_part = tiles // OUT_PARTS
    wide = group * HEAD_WIDTH // OUT_PARTS
    copies = []
    for h in range(local_heads):
        for p in range(OUT_PARTS):
            pl.loop(p * per_part, (p + 1) * per_part, unroll=unroll)(lambda i, h=h: visit(h, i))
            at = pl.ds((h * OUT_PARTS + p) * wide, wide)
            copies.append(pltpu.make_async_copy(o_ref.at[:, at], o_hbm.at[0, :, at], out_sem.at[h, p]))
            copies[-1].start()
    for copy in copies:
        copy.wait()


def mix_kernel(cols_x, group, w_ref, v_ref, acc_ref, live_ref, o_hbm, o_ref, out_sem):
    tile = HEADS_PER_TILE if group % HEADS_PER_TILE == 0 else 1
    height = tile * o_ref.shape[0]
    half = w_ref.shape[1]
    side = 1 - lax.rem(lax.axis_index("blk"), cols_x)
    other = pl.ds(pl.multiple_of(side * half, half), half)
    live = live_ref[...] > 0.0

    def visit(h, i):
        first = (h * group + i * tile) * HEAD_WIDTH
        kept = pl.ds(pl.multiple_of((h * (group // tile) + i) * height, height), height)
        values = with_ones(v_ref[other, h * HEAD_WIDTH : (h + 1) * HEAD_WIDTH])
        mixed = acc_ref[kept] + jnp.dot(w_ref[kept], values, preferred_element_type=jnp.float32)

        def cols(t):
            return pl.ds(pl.multiple_of(first + t * HEAD_WIDTH, HEAD_WIDTH), HEAD_WIDTH)

        store_heads(o_ref, mixed, live, cols, tile)

    in_parts(o_hbm, o_ref, out_sem, v_ref.shape[1] // HEAD_WIDTH, group, tile, visit, True)


def attend_kernel(
    rows_z, cols_x, group, spans, q_hbm, k_ref, v_ref, len_hbm, order_hbm, o_hbm,
    q_ref, o_ref, bias_ref, len_ref, order_ref, q_sem, small_sem, out_sem
):
    q_copy = pltpu.make_async_copy(q_hbm.at[0], q_ref, q_sem)
    len_copy = pltpu.make_async_copy(len_hbm, len_ref, small_sem.at[0])
    order_copy = pltpu.make_async_copy(order_hbm, order_ref, small_sem.at[1])
    for copy in (len_copy, order_copy, q_copy):
        copy.start()
    rows = q_ref.shape[0]
    chunks, _, chunk = bias_ref.shape
    len_copy.wait()
    order_copy.wait()
    row_pos = row_positions(order_ref, spans, rows)

    def fill(c):
        first = c * (chunk // rows)
        bias_ref[c] = mask(key_positions(order_ref, first, (1, chunk), rows_z, cols_x, spans, rows), row_pos)

    pl.loop(0, chunks)(fill)
    live = row_pos < len_ref[0]
    q_copy.wait()
    tile = HEADS_PER_TILE if group % HEADS_PER_TILE == 0 else 1
    height = tile * rows

    def visit(h, i):
        cols = slice(h * HEAD_WIDTH, (h + 1) * HEAD_WIDTH)
        q_cols, q = stacked_queries(q_ref, (h * group + i * tile) * HEAD_WIDTH, tile)

        def step(c, state):
            best, mixed = state
            at = pl.ds(pl.multiple_of(c * chunk, chunk), chunk)
            score = scores(q, k_ref[at, cols], bias_ref[c], tile)
            top = jnp.maximum(best, jnp.max(score, axis=1, keepdims=True))
            weight = jnp.exp2(score - top).astype(jnp.bfloat16)
            fresh = jnp.dot(weight, with_ones(v_ref[at, cols]), preferred_element_type=jnp.float32)
            return top, mixed * jnp.exp2(best - top) + fresh

        init = (
            jnp.full((height, 1), NEG_FILL, jnp.float32),
            jnp.zeros((height, 2 * HEAD_WIDTH), jnp.float32),
        )
        _, mixed = lax.fori_loop(0, chunks, step, init)
        store_heads(o_ref, mixed, live, q_cols, tile)

    in_parts(o_hbm, o_ref, out_sem, k_ref.shape[1] // HEAD_WIDTH, group, tile, visit, False)


def solution(mesh):
    blocks = mesh.shape["blk"]
    cols_x = row_length(blocks)
    rows_z = blocks // cols_x
    dma = pltpu.SemaphoreType.DMA
    hbm = pl.BlockSpec(memory_space=pltpu.HBM)
    vmem = pl.BlockSpec(memory_space=pltpu.VMEM)

    def shards(queries, keys, values, prompt_length, span_order):
        _, rows, width = queries.shape
        kv_width = keys.shape[2]
        local_heads = kv_width // HEAD_WIDTH
        group = width // kv_width
        total = blocks * rows
        chunk = min(total, KEY_CHUNK)
        spans = span_order.shape[0] // blocks
        queries, keys, values, span_order = (
            pltpu.with_memory_space_constraint(a, pltpu.HBM) for a in (queries, keys, values, span_order)
        )
        exchange_sems = [
            dma((2,)),
            pltpu.SemaphoreType.REGULAR((rows_z,)),
            pltpu.SemaphoreType.REGULAR((cols_x,)),
            dma((2,)),
            dma((2,)),
            dma((rows_z, 2)),
            dma((2,)),
        ]
        small = [pltpu.SMEM(prompt_length.shape, jnp.int32), pltpu.SMEM(span_order.shape, jnp.int32)]
        talk = pltpu.CompilerParams(collective_id=0, has_side_effects=True, vmem_limit_bytes=VMEM_LIMIT)
        quiet = pltpu.CompilerParams(vmem_limit_bytes=VMEM_LIMIT)
        out_shape = jax.ShapeDtypeStruct(queries.shape, queries.dtype)
        out_sems = dma((local_heads, OUT_PARTS))
        gathered = pltpu.VMEM((total, kv_width), keys.dtype)
        bias = pltpu.VMEM((total // chunk, rows, chunk), jnp.float32)
        wide = pltpu.VMEM((rows, width), queries.dtype)
        if chunk == total and cols_x == 2:
            queue = local_heads * group * rows
            half = total // 2
            parts = pl.pallas_call(
                functools.partial(pair_kernel, rows_z, cols_x, group, spans),
                out_shape=[
                    pltpu.VMEM((queue, half), jnp.bfloat16),
                    gathered,
                    pltpu.VMEM((queue, 2 * HEAD_WIDTH), jnp.float32),
                    pltpu.VMEM((rows, HEAD_WIDTH), jnp.float32),
                ],
                in_specs=[hbm] * 5,
                out_specs=[vmem] * 4,
                scratch_shapes=[
                    wide,
                    gathered,
                    pltpu.VMEM((queue, half), jnp.bfloat16),
                    pltpu.VMEM((queue, HEAD_WIDTH), jnp.float32),
                    pltpu.VMEM((2, rows, half), jnp.float32),
                    *small,
                    dma,
                    dma((2,)),
                    *exchange_sems,
                ],
                compiler_params=talk,
            )(keys, values, queries, prompt_length, span_order)
            return pl.pallas_call(
                functools.partial(mix_kernel, cols_x, group),
                out_shape=out_shape,
                in_specs=[vmem] * 4,
                out_specs=hbm,
                scratch_shapes=[wide, out_sems],
                compiler_params=quiet,
            )(*parts)
        k_all, v_all = pl.pallas_call(
            functools.partial(gather_kernel, rows_z, cols_x),
            out_shape=[gathered] * 2,
            in_specs=[hbm] * 2,
            out_specs=[vmem] * 2,
            scratch_shapes=exchange_sems,
            compiler_params=talk,
        )(keys, values)
        return pl.pallas_call(
            functools.partial(attend_kernel, rows_z, cols_x, group, spans),
            out_shape=out_shape,
            in_specs=[hbm, vmem, vmem, hbm, hbm],
            out_specs=hbm,
            scratch_shapes=[wide, wide, bias, *small, dma, dma((2,)), out_sems],
            compiler_params=quiet,
        )(queries, k_all, v_all, prompt_length, span_order)

    spec = P("rep", "blk", "head")
    return jax.shard_map(
        shards, mesh=mesh, in_specs=(spec, spec, spec, P("rep"), P("rep")), out_specs=spec, check_vma=False
    )
```

```python
import functools
import math

import jax
import jax.numpy as jnp
from jax import lax
from jax.experimental import pallas as pl
from jax.experimental.pallas import tpu as pltpu
from jax.sharding import PartitionSpec as P

HEAD_WIDTH = 128
NEG_FILL = -1e30
HEADS_PER_TILE = 2
KEY_CHUNK = 512
OUT_PARTS = 1
VMEM_LIMIT = 40 * 1024 * 1024
MESH = pl.DeviceIdType.MESH


def row_length(blocks):
    return max(d for d in range(1, math.isqrt(blocks) + 1) if blocks % d == 0)


def row_positions(order_ref, spans, rows):
    span = rows // spans
    index = lax.broadcasted_iota(jnp.int32, (rows, 1), 0)
    position = jnp.zeros((rows, 1), jnp.int32)
    for t in range(spans):
        first = order_ref[lax.axis_index("blk") * spans + t] * span
        position = jnp.where(index // span == t, first + index % span, position)
    return position


def key_positions(order_ref, first_block, shape, rows_z, cols_x, spans, rows):
    span = rows // spans
    index = lax.broadcasted_iota(jnp.int32, shape, 1)
    position = jnp.zeros(shape, jnp.int32)
    for t in range(shape[1] // span):
        slot = first_block + t // spans
        block = lax.rem(slot, rows_z) * cols_x + lax.div(slot, rows_z)
        first = order_ref[block * spans + t % spans] * span
        position = jnp.where(index // span == t, first + index % span, position)
    return position


def mask(key_pos, row_pos):
    return jnp.where(key_pos <= row_pos, 0.0, NEG_FILL)


def exchange(rows_z, cols_x, sources, refs, meanwhile, prepare, own_keys, own_sem, ready_z, ready_x, z_send, x_send, z_recv, x_recv):
    rows = sources[0].shape[1]
    me = lax.axis_index("blk")
    z, x = lax.div(me, cols_x), lax.rem(me, cols_x)
    even = lax.rem(z, 2) == 0
    first = lax.axis_index("head") == 0
    near = range(1, rows_z)
    far = range(rows_z - 1, 0, -1)
    own = pl.ds((x * rows_z + z) * rows, rows)
    loads = [pltpu.make_async_copy(sources[u].at[0], refs[u].at[own], own_sem.at[u]) for u in range(2)]
    for load in loads:
        load.start()
    meanwhile()

    def send(source, u, row, to_row, to_col, send_sem, recv_sem):
        at = pl.ds((x * rows_z + row) * rows, rows)
        return pltpu.make_async_remote_copy(
            src_ref=refs[u].at[at] if source is None else source,
            dst_ref=refs[u].at[at],
            send_sem=send_sem,
            recv_sem=recv_sem,
            device_id={"blk": to_row * cols_x + to_col},
            device_id_type=MESH,
        )

    def z_copy(row, to_row, u, source=None):
        return send(source, u, row, to_row, x, z_send.at[u], z_recv.at[row - jnp.where(row > to_row, 1, 0), u])

    def x_copy(row, col, u):
        return send(None, u, row, z, col, x_send.at[u], x_recv.at[u])

    def above(d, visit):
        pl.when(z + d < rows_z)(lambda: visit(z + d))

    def below(d, visit):
        pl.when(z >= d)(lambda: visit(z - d))

    def right(visit):
        for e in range(1, cols_x):
            pl.when(x + e < cols_x)(lambda e=e: visit(x + e))

    def left(visit):
        for e in range(1, cols_x):
            pl.when(x >= e)(lambda e=e: visit(x - e))

    def spread(row, u):
        for e in range(1, cols_x):
            x_copy(row, lax.rem(x + e, cols_x), u).start()

    def signal(sem, row, col):
        pl.semaphore_signal(sem, inc=1, device_id={"blk": row * cols_x + col}, device_id_type=MESH)

    barrier = pltpu.get_barrier_semaphore()
    for d in near:
        above(d, lambda row: signal(barrier, row, x))
    right(lambda col: signal(barrier, z, col))
    pl.when(z + x > 0)(lambda: pl.semaphore_wait(barrier, z + x))
    for d in far:
        below(d, lambda row: signal(ready_z.at[z - 1], row, x))
    left(lambda col: signal(ready_x.at[x - 1], z, col))

    def straight(u):
        return first & (u == 1)

    def send_below(u):
        for d in far:
            go = functools.partial(below, d, lambda row: z_copy(z, row, u, sources[u].at[0]).start())
            if d == 2:
                pl.when(even | straight(u))(go)
            else:
                go()

    def send_above(d, *which):
        for u in which:
            go = functools.partial(above, d, lambda row, u=u: z_copy(z, row, u, sources[u].at[0]).start())
            if d == 2:
                pl.when(even)(go)
            elif d == 3:
                pl.when(straight(u))(go)
            else:
                go()

    def answered(d):
        above(d, lambda row: pl.semaphore_wait(ready_z.at[row - 1], 1))

    def relay_from_below(d, u):
        def take(row):
            z_copy(row, z, u).wait_recv()
            if d == 1:
                pl.when(even & (z + 1 < rows_z))(lambda: z_copy(row, z + 1, u).start())
            if d == 2:
                pl.when((z + 1 < rows_z) & ~straight(u))(lambda: z_copy(row, z + 1, u).start())
            spread(row, u)

        below(d, take)

    def relay_from_above(d, u):
        def take(row):
            z_copy(row, z, u).wait_recv()
            spread(row, u)
            if d == 1:
                pl.when(even & (z >= 1) & ~straight(u))(lambda: z_copy(row, z - 1, u).start())

        above(d, take)

    def relay(d, u):
        relay_from_below(d, u)
        relay_from_above(d, u)

    def send_left(u):
        loads[u].wait()
        left(lambda col: x_copy(z, col, u).start())

    def send_right(*which):
        right(lambda col: pl.semaphore_wait(ready_x.at[col - 1], 1))
        for u in which:
            right(lambda col: x_copy(z, col, u).start())

    def eager():
        for u in range(2):
            send_below(u)
            send_left(u)
        send_right(0, 1)
        for d in near:
            answered(d)
            send_above(d, 0, 1)

    def patient():
        send_below(0)
        send_left(0)
        send_left(1)
        send_right(0, 1)
        for d in near:
            answered(d)
            send_above(d, 0)

    pl.when(first)(eager)
    pl.when(~first)(patient)
    prepare()
    lowest = first & (z == 0)
    upper = first & (z > 0)

    def values_now():
        send_below(1)
        for d in near:
            send_above(d, 1)

    for d in near:
        relay(d, 0)
        if d == 1:
            pl.when(lowest)(lambda: relay_from_above(1, 1))
            pl.when(upper)(lambda: relay_from_below(1, 1))
            pl.when(~first)(values_now)
    pl.when(~upper)(lambda: relay_from_below(1, 1))
    for d in near[1:]:
        relay_from_below(d, 1)
    pl.when(~lowest)(lambda: relay_from_above(1, 1))
    for d in near[1:]:
        relay_from_above(d, 1)
    own_keys()

    def many(u, count, sem):
        at = pl.ds(0, count * rows)
        return pltpu.make_async_copy(refs[u].at[at], refs[u].at[at], sem)

    along_x = (cols_x - 1) * rows_z

    def arrived(u):
        many(u, along_x, x_recv.at[u]).wait()

    def sent_along_z(row, detours):
        odd, inside = row % 2 == 1, 0 < row < rows_z - 1
        count = rows_z - 1 - (odd and row + 2 < rows_z) + (not odd and inside)
        if detours:
            count += (row >= 2 and row + 1 < rows_z) - (row + 3 < rows_z)
            count += (not odd and inside) - (odd and row >= 2)
        return count

    def drain():
        for u in range(2):
            many(u, along_x, x_send.at[u]).wait()
            for row in range(rows_z):
                for detours in (True, False):
                    here = (z == row) & (straight(u) != detours)
                    count = sent_along_z(row, detours)
                    pl.when(here)(lambda u=u, count=count: many(u, count, z_send.at[u]).wait())

    return arrived, drain


def gather_kernel(rows_z, cols_x, k_hbm, v_hbm, k_ref, v_ref, *sems):
    arrived, drain = exchange(rows_z, cols_x, (k_hbm, v_hbm), (k_ref, v_ref), *[lambda: None] * 3, *sems)
    arrived(0)
    arrived(1)
    drain()


def stacked_queries(q_ref, first, tile):
    def cols(t):
        return pl.ds(pl.multiple_of(first + t * HEAD_WIDTH, HEAD_WIDTH), HEAD_WIDTH)

    return cols, jnp.concatenate([q_ref[:, cols(t)] for t in range(tile)], axis=0)


def scores(q, keys, bias, tile):
    scale = HEAD_WIDTH ** (-0.5) * math.log2(math.e)
    score = lax.dot_general(q, keys, (((1,), (1,)), ((), ())), preferred_element_type=jnp.float32)
    rows, chunk = bias.shape
    return ((score * scale).reshape(tile, rows, chunk) + bias[None]).reshape(tile * rows, chunk)


def pair_kernel(
    rows_z, cols_x, group, spans, k_hbm, v_hbm, q_hbm, len_hbm, order_hbm, w_ref, v_ref, acc_ref, live_ref,
    q_ref, k_ref, own_w_ref, top_ref, bias_ref, len_ref, order_ref, q_sem, small_sem, *sems
):
    rows = q_ref.shape[0]
    half = rows_z * rows
    x = lax.rem(lax.axis_index("blk"), cols_x)
    own, other = (pl.ds(pl.multiple_of(side * half, half), half) for side in (x, 1 - x))
    q_copy = pltpu.make_async_copy(q_hbm.at[0], q_ref, q_sem)
    len_copy = pltpu.make_async_copy(len_hbm, len_ref, small_sem.at[0])
    order_copy = pltpu.make_async_copy(order_hbm, order_ref, small_sem.at[1])
    copies = (len_copy, order_copy, q_copy)
    tile = HEADS_PER_TILE if group % HEADS_PER_TILE == 0 else 1
    height = tile * rows
    tiles = group // tile

    def prepare():
        for copy in copies:
            copy.wait()
        row_pos = row_positions(order_ref, spans, rows)
        for n, side in enumerate((x, 1 - x)):
            key_pos = key_positions(order_ref, side * rows_z, (1, half), rows_z, cols_x, spans, rows)
            bias_ref[n] = mask(key_pos, row_pos)
        live_ref[...] = jnp.broadcast_to(jnp.where(row_pos < len_ref[0], 1.0, 0.0), live_ref.shape)

    def each_tile(visit):
        for h in range(k_ref.shape[1] // HEAD_WIDTH):

            def go(i, h=h):
                kept = pl.ds(pl.multiple_of((h * tiles + i) * height, height), height)
                visit(h * tiles + i, kept, slice(h * HEAD_WIDTH, (h + 1) * HEAD_WIDTH))

            pl.loop(0, tiles, unroll=True)(go)

    def own_keys():
        def visit(n, kept, cols):
            _, q = stacked_queries(q_ref, n * tile * HEAD_WIDTH, tile)
            score = scores(q, k_ref[own, cols], bias_ref[0], tile)
            top = jnp.max(score, axis=1, keepdims=True)
            own_w_ref[kept] = jnp.exp2(score - top).astype(jnp.bfloat16)
            top_ref[kept] = jnp.broadcast_to(top, (height, HEAD_WIDTH))

        each_tile(visit)

    arrived, drain = exchange(
        rows_z, cols_x, (k_hbm, v_hbm), (k_ref, v_ref), lambda: [copy.start() for copy in copies], prepare, own_keys,
        *sems
    )

    def own_values(n, kept, cols):
        acc_ref[kept] = jnp.dot(own_w_ref[kept], with_ones(v_ref[own, cols]), preferred_element_type=jnp.float32)

    each_tile(own_values)
    arrived(0)

    def other_keys(n, kept, cols):
        _, q = stacked_queries(q_ref, n * tile * HEAD_WIDTH, tile)
        score = scores(q, k_ref[other, cols], bias_ref[1], tile)
        best = top_ref[kept]
        top = jnp.maximum(best, jnp.max(score, axis=1, keepdims=True))
        wide_top = jnp.concatenate([top] * (half // HEAD_WIDTH), axis=1)
        w_ref[kept] = jnp.exp2(score - wide_top).astype(jnp.bfloat16)
        fade = jnp.exp2(best - top)
        acc_ref[kept] = acc_ref[kept] * jnp.concatenate([fade, fade], axis=1)

    each_tile(other_keys)
    arrived(1)
    drain()


def store_heads(o_ref, mixed, live, cols, tile):
    rows = live.shape[0]
    out = mixed[:, :HEAD_WIDTH] / mixed[:, HEAD_WIDTH:]
    for t in range(tile):
        o_ref[:, cols(t)] = jnp.where(live, out[t * rows : (t + 1) * rows], 0.0).astype(o_ref.dtype)


def with_ones(values):
    return jnp.concatenate([values, jnp.ones((values.shape[0], HEAD_WIDTH), values.dtype)], axis=1)


def in_parts(o_hbm, o_ref, out_sem, local_heads, group, tile, visit, unroll):
    tiles = group // tile
    per_part = tiles // OUT_PARTS
    wide = group * HEAD_WIDTH // OUT_PARTS
    copies = []
    for h in range(local_heads):
        for p in range(OUT_PARTS):
            pl.loop(p * per_part, (p + 1) * per_part, unroll=unroll)(lambda i, h=h: visit(h, i))
            at = pl.ds((h * OUT_PARTS + p) * wide, wide)
            copies.append(pltpu.make_async_copy(o_ref.at[:, at], o_hbm.at[0, :, at], out_sem.at[h, p]))
            copies[-1].start()
    for copy in copies:
        copy.wait()


def mix_kernel(cols_x, group, w_ref, v_ref, acc_ref, live_ref, o_hbm, o_ref, out_sem):
    tile = HEADS_PER_TILE if group % HEADS_PER_TILE == 0 else 1
    height = tile * o_ref.shape[0]
    half = w_ref.shape[1]
    side = 1 - lax.rem(lax.axis_index("blk"), cols_x)
    other = pl.ds(pl.multiple_of(side * half, half), half)
    live = live_ref[...] > 0.0

    def visit(h, i):
        first = (h * group + i * tile) * HEAD_WIDTH
        kept = pl.ds(pl.multiple_of((h * (group // tile) + i) * height, height), height)
        values = with_ones(v_ref[other, h * HEAD_WIDTH : (h + 1) * HEAD_WIDTH])
        mixed = acc_ref[kept] + jnp.dot(w_ref[kept], values, preferred_element_type=jnp.float32)

        def cols(t):
            return pl.ds(pl.multiple_of(first + t * HEAD_WIDTH, HEAD_WIDTH), HEAD_WIDTH)

        store_heads(o_ref, mixed, live, cols, tile)

    in_parts(o_hbm, o_ref, out_sem, v_ref.shape[1] // HEAD_WIDTH, group, tile, visit, True)


def attend_kernel(
    rows_z, cols_x, group, spans, q_hbm, k_ref, v_ref, len_hbm, order_hbm, o_hbm,
    q_ref, o_ref, bias_ref, len_ref, order_ref, q_sem, small_sem, out_sem
):
    q_copy = pltpu.make_async_copy(q_hbm.at[0], q_ref, q_sem)
    len_copy = pltpu.make_async_copy(len_hbm, len_ref, small_sem.at[0])
    order_copy = pltpu.make_async_copy(order_hbm, order_ref, small_sem.at[1])
    for copy in (len_copy, order_copy, q_copy):
        copy.start()
    rows = q_ref.shape[0]
    chunks, _, chunk = bias_ref.shape
    len_copy.wait()
    order_copy.wait()
    row_pos = row_positions(order_ref, spans, rows)

    def fill(c):
        first = c * (chunk // rows)
        bias_ref[c] = mask(key_positions(order_ref, first, (1, chunk), rows_z, cols_x, spans, rows), row_pos)

    pl.loop(0, chunks)(fill)
    live = row_pos < len_ref[0]
    q_copy.wait()
    tile = HEADS_PER_TILE if group % HEADS_PER_TILE == 0 else 1
    height = tile * rows

    def visit(h, i):
        cols = slice(h * HEAD_WIDTH, (h + 1) * HEAD_WIDTH)
        q_cols, q = stacked_queries(q_ref, (h * group + i * tile) * HEAD_WIDTH, tile)

        def step(c, state):
            best, mixed = state
            at = pl.ds(pl.multiple_of(c * chunk, chunk), chunk)
            score = scores(q, k_ref[at, cols], bias_ref[c], tile)
            top = jnp.maximum(best, jnp.max(score, axis=1, keepdims=True))
            weight = jnp.exp2(score - top).astype(jnp.bfloat16)
            fresh = jnp.dot(weight, with_ones(v_ref[at, cols]), preferred_element_type=jnp.float32)
            return top, mixed * jnp.exp2(best - top) + fresh

        init = (
            jnp.full((height, 1), NEG_FILL, jnp.float32),
            jnp.zeros((height, 2 * HEAD_WIDTH), jnp.float32),
        )
        _, mixed = lax.fori_loop(0, chunks, step, init)
        store_heads(o_ref, mixed, live, q_cols, tile)

    in_parts(o_hbm, o_ref, out_sem, k_ref.shape[1] // HEAD_WIDTH, group, tile, visit, False)


def solution(mesh):
    blocks = mesh.shape["blk"]
    cols_x = row_length(blocks)
    rows_z = blocks // cols_x
    dma = pltpu.SemaphoreType.DMA
    hbm = pl.BlockSpec(memory_space=pltpu.HBM)
    vmem = pl.BlockSpec(memory_space=pltpu.VMEM)

    def shards(queries, keys, values, prompt_length, span_order):
        _, rows, width = queries.shape
        kv_width = keys.shape[2]
        local_heads = kv_width // HEAD_WIDTH
        group = width // kv_width
        total = blocks * rows
        chunk = min(total, KEY_CHUNK)
        spans = span_order.shape[0] // blocks
        queries, keys, values, span_order = (
            pltpu.with_memory_space_constraint(a, pltpu.HBM) for a in (queries, keys, values, span_order)
        )
        exchange_sems = [
            dma((2,)),
            pltpu.SemaphoreType.REGULAR((max(rows_z - 1, 1),)),
            pltpu.SemaphoreType.REGULAR((max(cols_x - 1, 1),)),
            dma((2,)),
            dma((2,)),
            dma((max(rows_z - 1, 1), 2)),
            dma((2,)),
        ]
        small = [pltpu.SMEM(prompt_length.shape, jnp.int32), pltpu.SMEM(span_order.shape, jnp.int32)]
        talk = pltpu.CompilerParams(collective_id=0, has_side_effects=True, vmem_limit_bytes=VMEM_LIMIT)
        quiet = pltpu.CompilerParams(vmem_limit_bytes=VMEM_LIMIT)
        out_shape = jax.ShapeDtypeStruct(queries.shape, queries.dtype)
        out_sems = dma((local_heads, OUT_PARTS))
        gathered = pltpu.VMEM((total, kv_width), keys.dtype)
        bias = pltpu.VMEM((total // chunk, rows, chunk), jnp.float32)
        wide = pltpu.VMEM((rows, width), queries.dtype)
        if chunk == total and cols_x == 2:
            queue = local_heads * group * rows
            half = total // 2
            parts = pl.pallas_call(
                functools.partial(pair_kernel, rows_z, cols_x, group, spans),
                out_shape=[
                    pltpu.VMEM((queue, half), jnp.bfloat16),
                    gathered,
                    pltpu.VMEM((queue, 2 * HEAD_WIDTH), jnp.float32),
                    pltpu.VMEM((rows, HEAD_WIDTH), jnp.float32),
                ],
                in_specs=[hbm] * 5,
                out_specs=[vmem] * 4,
                scratch_shapes=[
                    wide,
                    gathered,
                    pltpu.VMEM((queue, half), jnp.bfloat16),
                    pltpu.VMEM((queue, HEAD_WIDTH), jnp.float32),
                    pltpu.VMEM((2, rows, half), jnp.float32),
                    *small,
                    dma,
                    dma((2,)),
                    *exchange_sems,
                ],
                compiler_params=talk,
            )(keys, values, queries, prompt_length, span_order)
            return pl.pallas_call(
                functools.partial(mix_kernel, cols_x, group),
                out_shape=out_shape,
                in_specs=[vmem] * 4,
                out_specs=hbm,
                scratch_shapes=[wide, out_sems],
                compiler_params=quiet,
            )(*parts)
        k_all, v_all = pl.pallas_call(
            functools.partial(gather_kernel, rows_z, cols_x),
            out_shape=[gathered] * 2,
            in_specs=[hbm] * 2,
            out_specs=[vmem] * 2,
            scratch_shapes=exchange_sems,
            compiler_params=talk,
        )(keys, values)
        return pl.pallas_call(
            functools.partial(attend_kernel, rows_z, cols_x, group, spans),
            out_shape=out_shape,
            in_specs=[hbm, vmem, vmem, hbm, hbm],
            out_specs=hbm,
            scratch_shapes=[wide, wide, bias, *small, dma, dma((2,)), out_sems],
            compiler_params=quiet,
        )(queries, k_all, v_all, prompt_length, span_order)

    spec = P("rep", "blk", "head")
    return jax.shard_map(
        shards, mesh=mesh, in_specs=(spec, spec, spec, P("rep"), P("rep")), out_specs=spec, check_vma=False
    )
```
